8 devices in a mesh: rep: 4 (over z, y, x), nodes: 2 (over core).
Axes of the slice: x: 2, y: 2, z: 1, core: 2. Of those that a mesh axis runs over, the one named last changes fastest.
Arguments:
- adjacency: bfloat16 [4, 4096, 16384], P(None, 'nodes', 'rep')
- features: bfloat16 [16384, 602], P(('rep', 'nodes'))
- w_one: float32 [602, 128], replicated
- w_two: float32 [128, 41], replicated
- labels: int32 [16384], P(('rep', 'nodes'))
- label_mask: int32 [16384], P(('rep', 'nodes'))
Outputs:
- output 1: float32 [], replicated
- output 2: float32 [602, 128], replicated
- output 3: float32 [128, 41], replicated
All inputs are finite; a program needn't handle non-finite values.
Results may differ from the reference program's by a relative error of at most 0.001.
Values are sent between devices in bfloat16 or wider.
A program may use at most 1 GiB of HBM per device.

```python
import jax
import jax.numpy as jnp
from jax import lax

REPLICAS = 4
NODE_GROUP = 2
ROWS_DEV = 2048
F_IN = 602
F_HID = 128
N_CLASS = 41
N_COMM = 16

N_TOTAL = ROWS_DEV * REPLICAS * NODE_GROUP


def make_adjacency(edge_key, community):
    col_ids = jnp.arange(N_TOTAL)

    def one_block(block_id):
        row_ids = block_id * ROWS_DEV + jnp.arange(ROWS_DEV)
        coin_draw = jax.random.randint(jax.random.fold_in(edge_key, block_id), (ROWS_DEV, N_TOTAL), 0, 1000)
        comm_rows = lax.dynamic_slice(community, (block_id * ROWS_DEV,), (ROWS_DEV,))
        same_comm = comm_rows[:, None] == community[None, :]
        has_edge = (coin_draw < jnp.where(same_comm, 500, 40)) | (row_ids[:, None] == col_ids[None, :])
        degree = jnp.sum(has_edge.astype(jnp.int32), axis=1)
        return (has_edge.astype(jnp.float32) / degree[:, None].astype(jnp.float32)).astype(jnp.bfloat16)

    row_blocks = lax.map(one_block, jnp.arange(N_TOTAL // ROWS_DEV))
    return row_blocks.reshape(REPLICAS, N_TOTAL // REPLICAS, N_TOTAL)


def setup_inputs(seed: int = 0) -> dict:
    base_key = jax.random.key(seed)
    key_list = jax.random.split(base_key, 8)
    community = jax.random.randint(key_list[0], (N_TOTAL,), 0, N_COMM)
    adjacency = make_adjacency(key_list[1], community)
    comm_embed = jax.random.normal(key_list[2], (N_COMM, F_IN), jnp.float32)
    feat_noise = 0.5 * jax.random.normal(key_list[3], (N_TOTAL, F_IN), jnp.float32)
    features = (comm_embed[community] + feat_noise).astype(jnp.bfloat16)
    w_one = jax.random.normal(key_list[4], (F_IN, F_HID), jnp.float32) * F_IN ** -0.5
    w_two = 2.0 * jax.random.normal(key_list[5], (F_HID, N_CLASS), jnp.float32) * F_HID ** -0.5
    labels = jax.random.randint(key_list[6], (N_TOTAL,), 0, N_CLASS).astype(jnp.int32)
    mask_draw = jax.random.randint(key_list[7], (N_TOTAL,), 0, 10)
    label_mask = jnp.where((mask_draw < 6) | (jnp.arange(N_TOTAL) == 0), 1, 0).astype(jnp.int32)
    return {"adjacency": adjacency, "features": features, "w_one": w_one, "w_two": w_two, "labels": labels, "label_mask": label_mask}


def reference(adjacency, features, w_one, w_two, labels, label_mask):
    node_count = features.shape[0]
    adj_flat = adjacency.reshape(node_count, node_count)
    w_one_lo = w_one.astype(jnp.bfloat16)
    w_two_lo = w_two.astype(jnp.bfloat16)
    y_one = jnp.dot(features, w_one_lo, preferred_element_type=jnp.float32).astype(jnp.bfloat16)
    z_one = jnp.dot(adj_flat, y_one, preferred_element_type=jnp.float32)
    h_one = jnp.maximum(z_one, 0.0).astype(jnp.bfloat16)
    y_two = jnp.dot(h_one, w_two_lo, preferred_element_type=jnp.float32).astype(jnp.bfloat16)
    z_two = jnp.dot(adj_flat, y_two, preferred_element_type=jnp.float32)
    weights = label_mask.astype(jnp.float32)
    label_count = jnp.sum(weights)
    log_probs = jax.nn.log_softmax(z_two, axis=-1)
    one_hot = (labels[:, None] == jnp.arange(N_CLASS)[None, :]).astype(jnp.float32)
    loss_value = -jnp.sum(weights * jnp.sum(one_hot * log_probs, axis=-1)) / label_count
    g_two = ((jnp.exp(log_probs) - one_hot) * (weights / label_count)[:, None]).astype(jnp.bfloat16)
    dy_two = lax.dot_general(adj_flat, g_two, (((0,), (0,)), ((), ())), preferred_element_type=jnp.float32).astype(jnp.bfloat16)
    dw_two = lax.dot_general(h_one, dy_two, (((0,), (0,)), ((), ())), preferred_element_type=jnp.float32)
    dh_one = lax.dot_general(dy_two, w_two_lo, (((1,), (1,)), ((), ())), preferred_element_type=jnp.float32)
    g_one = jnp.where(z_one > 0.0, dh_one, 0.0).astype(jnp.bfloat16)
    dy_one = lax.dot_general(adj_flat, g_one, (((0,), (0,)), ((), ())), preferred_element_type=jnp.float32).astype(jnp.bfloat16)
    dw_one = lax.dot_general(features, dy_one, (((0,), (0,)), ((), ())), preferred_element_type=jnp.float32)
    return (loss_value, dw_one, dw_two)
```

```python
import jax
import jax.numpy as jnp
from jax import lax
from jax.experimental import pallas as pl
from jax.experimental.pallas import tpu as pltpu
from jax.sharding import PartitionSpec as P

BF = jnp.bfloat16
F32 = jnp.float32
MESH = pl.DeviceIdType.MESH

CH = 256
NCH = 8
CP = 48
L2, L3, L4 = 2, 4, 5
M1, M2, M3 = 1, 2, 3
N1 = 1


def mm(a, b, ca=1, cb=0):
    return lax.dot_general(a, b, (((ca,), (cb,)), ((), ())), preferred_element_type=F32)


def kernel(
    n_class, adj, feat, w1, w2, lab, loss_o, dw1_o, dw2_o,
    a_s, x_s, w2n, w2t, y1, p1, p1r1, p1r2, h1t, y2, zacc, zs, zr1, zr2, g2, dacc, drec, g1, eacc, erec,
    cnt, cntr, f2, f2r, fw, fr0, fs, fr1, fr2, fo, lossv,
    a_sem, x_sem, y1_ss, y1_rs, p1_ss, p1_rs, y2_ss, y2_rs, z_ss, z_rs, g2_ss, g2_rs, g1_ss, g1_rs,
    d_ss, d_rs, c_ss, c_rs, f2_ss, f2_rs, fw_ss, fw_rs,
):
    r = lax.axis_index("rep")
    i = lax.axis_index("nodes")
    nbx = r + 1 - 2 * (r % 2)
    nby = (r + 2) % 4
    r0, r1 = r % 2, r // 2
    other = 1 - i

    def near(e):
        return nbx * (1 - e) + nby * e

    def far(e):
        return nby * (1 - e) + nbx * e

    def place(a, e):
        d0 = (r0 + a % 2) % 2
        d1 = (r1 + a // 2) % 2
        return 3 * (1 - d0) * (1 - d1) + d0 * (1 - d1) * (1 + e) + (1 - d0) * d1 * (2 - e)

    def remote(src, dst, ss, rs, rep, core):
        return pltpu.make_async_remote_copy(
            src_ref=src, dst_ref=dst, send_sem=ss, recv_sem=rs, device_id=(rep, core), device_id_type=MESH
        )

    def rows_copy(chunk, slot):
        return pltpu.make_async_copy(
            adj.at[:, pl.ds(pl.multiple_of(chunk * CH, CH), CH), :], a_s.at[slot], a_sem.at[slot]
        )

    def cols_start(k, slot):
        @pl.loop(0, NCH)
        def _(g):
            for core in range(2):
                pltpu.make_async_copy(
                    adj.at[:, pl.ds(pl.multiple_of(g * CH, CH), CH), pl.ds(pl.multiple_of(core * 2048 + k * CH, CH), CH)],
                    a_s.at[slot, :, :, pl.ds(pl.multiple_of(g * 2 * CH + core * CH, CH), CH)],
                    a_sem.at[slot],
                ).start()

    x_copy = pltpu.make_async_copy(feat, x_s, x_sem)
    x_copy.start()
    rows_copy(0, 0).start()
    rows_copy(1, 1).start()
    cols_start(0, 2)
    cols_start(1, 3)

    barrier = pltpu.get_barrier_semaphore()
    pl.semaphore_signal(barrier, inc=1, device_id=(nbx, i), device_id_type=MESH)
    pl.semaphore_signal(barrier, inc=1, device_id=(nby, i), device_id_type=MESH)
    pl.semaphore_signal(barrier, inc=1, device_id=(r, other), device_id_type=MESH)

    w2n[...] = jnp.zeros_like(w2n)
    w2n[:, 0:n_class] = w2[...]
    w2t[...] = jnp.transpose(w2n[...], (1, 0)).astype(BF)
    zacc[...] = jnp.zeros_like(zacc)
    dacc[...] = jnp.zeros_like(dacc)
    eacc[...] = jnp.zeros_like(eacc)
    lossv[...] = jnp.zeros_like(lossv)
    f2[0] = jnp.zeros_like(f2[0])
    mask_all = jnp.where(lab[...] >= 0, 1.0, 0.0).astype(F32)
    total = jnp.sum(jnp.sum(mask_all, axis=0, keepdims=True), axis=1, keepdims=True)
    cnt[0] = jnp.broadcast_to(total, (8, 128))
    w1b = w1[...].astype(BF)
    pl.semaphore_wait(barrier, 3)

    def cnt_copy(n):
        rep = (nbx, nby, r)[n]
        core = (i, i, other)[n]
        return remote(cnt.at[n], cntr.at[n], c_ss.at[n], c_rs.at[n], rep, core)

    cnt_copy(0).start()
    x_copy.wait()

    def y1_copy(b):
        part = y1.at[i, pl.ds(pl.multiple_of(b * 512, 512), 512), :]
        return remote(part, part, y1_ss.at[b], y1_rs.at[b], r, other)

    def y1_recv(b):
        part = y1.at[other, pl.ds(pl.multiple_of(b * 512, 512), 512), :]
        return remote(part, part, y1_ss.at[b], y1_rs.at[b], r, other)

    @pl.loop(0, 4)
    def _(b):
        rows = pl.ds(pl.multiple_of(b * 512, 512), 512)
        y1[i, rows, :] = mm(x_s[rows, :], w1b).astype(BF)
        y1_copy(b).start()

    cnt_copy(0).wait_recv()
    cnt[1] = cnt[0] + cntr[0]
    cnt_copy(1).start()

    @pl.loop(0, 4)
    def _(b):
        y1_recv(b).wait_recv()

    def p1_first(c, e):
        return remote(p1.at[c, pl.ds(0, 2)], p1r1.at[c], p1_ss.at[0, c], p1_rs.at[0, c], near(e), i)

    def p1_second(c, e):
        return remote(p1.at[c, 2], p1r2.at[c], p1_ss.at[1, c], p1_rs.at[1, c], far(e), i)

    def y2_copy(c):
        return remote(y2.at[c, i], y2.at[c, i], y2_ss.at[c], y2_rs.at[c], r, other)

    def y2_recv(c):
        return remote(y2.at[c, other], y2.at[c, other], y2_ss.at[c], y2_rs.at[c], r, other)

    def z_part(lhs, slot, g):
        rhs = a_s[slot, :, :, pl.ds(pl.multiple_of(g * 2 * CH, 2 * CH), 2 * CH)].reshape(4 * CH, 2 * CH)
        return mm(lhs, rhs, 1, 1)

    def pass2_lhs(k):
        return jnp.concatenate([y2[k, 0], y2[k, 1]], axis=1)

    @pl.loop(0, NCH - 1 + L4)
    def _(t):
        @pl.when(t < NCH)
        def _():
            c = t
            e = c % 2
            rows_copy(c, e).wait()
            res = mm(a_s[e].reshape(4 * CH, 4096), y1[...].reshape(4096, 128))
            for a in range(4):
                p1[c, place(a, e)] = res[a * CH:(a + 1) * CH]
            p1_first(c, e).start()

            @pl.when(c + 2 < NCH)
            def _():
                rows_copy(c + 2, e).start()

        @pl.when(jnp.logical_and(t >= L2, t < NCH + L2))
        def _():
            c = t - L2
            e = c % 2
            p1_first(c, e).wait_recv()
            p1[c, 2] = p1[c, 2] + p1r1[c, 0]
            p1_second(c, e).start()
            p1[c, 3] = p1[c, 3] + p1r1[c, 1]

        @pl.when(jnp.logical_and(t >= L3, t < NCH + L3))
        def _():
            c = t - L3
            e = c % 2
            p1_second(c, e).wait_recv()
            h = jnp.maximum(p1[c, 3] + p1r2[c], 0.0)
            ht = jnp.transpose(h, (1, 0)).astype(BF)
            h1t[c] = ht
            y2[c, i] = mm(w2t[...], ht).astype(BF)
            y2_copy(c).start()

        @pl.when(t >= L4)
        def _():
            k = t - L4
            slot = 2 + k % 2
            y2_recv(k).wait_recv()
            rows_copy(0, slot).wait()
            lhs = pass2_lhs(k)

            @pl.loop(0, 2)
            def _(gg):
                for g4 in range(4):
                    g = gg * 4 + g4
                    zacc[g] = zacc[g] + z_part(lhs, slot, g)

            @pl.when(k + 2 < NCH)
            def _():
                cols_start(k + 2, slot)

            @pl.when(k + 2 == NCH)
            def _():
                rows_copy(0, 2).start()

    def z_first(q, e):
        return remote(zs.at[q, pl.ds(0, 2)], zr1.at[q], z_ss.at[0, q], z_rs.at[0, q], near(e), i)

    def z_second(q, e):
        return remote(zs.at[q, 2], zr2.at[q], z_ss.at[1, q], z_rs.at[1, q], far(e), i)

    def spread_first(buf, ss, rs, q, e):
        return remote(buf.at[q, 3], buf.at[q, 2], ss.at[0, q], rs.at[0, q], far(e), i)

    def spread_second(buf, ss, rs, q, e):
        return remote(buf.at[q, pl.ds(2, 2)], buf.at[q, pl.ds(0, 2)], ss.at[1, q], rs.at[1, q], near(e), i)

    y2_recv(NCH - 1).wait_recv()
    rows_copy(0, 3).wait()
    lhs_last = pass2_lhs(NCH - 1)

    @pl.loop(0, NCH)
    def _(q):
        g = (q + 6) % NCH
        e = q % 2
        z = zacc[g] + z_part(lhs_last, 3, g)
        for a in range(4):
            zs[q, place(a, e)] = z[:, a * CH:(a + 1) * CH]
        z_first(q, e).start()

    rows_copy(1, 3).start()
    cnt_copy(1).wait_recv()
    cnt[2] = cnt[1] + cntr[1]
    cnt_copy(2).start()
    cnt_copy(2).wait_recv()
    count = (cnt[2] + cntr[2])[0:1, 0:1]
    class_id = lax.broadcasted_iota(jnp.int32, (CP, CH), 0)

    def gathered(buf, q, e):
        return jnp.concatenate([buf[q, place(a, e)] for a in range(4)], axis=1)

    def half(core):
        return pl.ds(pl.multiple_of(core * 2048, 2048), 2048)

    def pair_copy(src, dst, n):
        return remote(src.at[:, half(other)], dst, d_ss.at[n], d_rs.at[n], r, other)

    @pl.loop(0, NCH + M3)
    def _(t):
        @pl.when(t < NCH)
        def _():
            q = t
            e = q % 2
            z_first(q, e).wait_recv()
            zs[q, 2] = zs[q, 2] + zr1[q, 0]
            z_second(q, e).start()
            zs[q, 3] = zs[q, 3] + zr1[q, 1]

        @pl.when(jnp.logical_and(t >= M1, t < NCH + M1))
        def _():
            q = t - M1
            e = q % 2
            z_second(q, e).wait_recv()
            z = jnp.where(class_id < n_class, zs[q, 3] + zr2[q], -1e30)
            top = jnp.max(z, axis=0, keepdims=True)
            shifted = z - top
            log_p = shifted - jnp.log(jnp.sum(jnp.exp(shifted), axis=0, keepdims=True))
            label = lab[pl.ds((q + 6) % NCH, 1), :]
            weight = jnp.where(label >= 0, 1.0, 0.0).astype(F32)
            hit = class_id == label
            lossv[...] = lossv[...] - weight * jnp.sum(jnp.where(hit, log_p, 0.0), axis=0, keepdims=True)
            prob = jnp.exp(log_p)
            g2[q, 3] = ((prob - jnp.where(hit, 1.0, 0.0)) * (weight / count)).astype(BF)
            spread_first(g2, g2_ss, g2_rs, q, e).start()

        @pl.when(jnp.logical_and(t >= M2, t < NCH + M2))
        def _():
            q = t - M2
            e = q % 2
            spread_first(g2, g2_ss, g2_rs, q, e).wait_recv()
            spread_second(g2, g2_ss, g2_rs, q, e).start()

        @pl.when(t >= M3)
        def _():
            q = t - M3
            e = q % 2
            slot = q % 4
            spread_second(g2, g2_ss, g2_rs, q, e).wait_recv()

            @pl.when(q >= 2)
            def _():
                rows_copy(0, slot).wait()

            lhs = gathered(g2, q, e)
            dacc[:, half(other)] += mm(lhs, a_s[slot, :, :, half(other)].reshape(4 * CH, 2048))

            @pl.when(q == NCH - 1)
            def _():
                pair_copy(dacc, drec, 0).start()

            dacc[:, half(i)] += mm(lhs, a_s[slot, :, :, half(i)].reshape(4 * CH, 2048))

            @pl.when(q < 4)
            def _():
                rows_copy((q + 10) % NCH, slot).start()

    pair_copy(dacc, drec, 0).wait_recv()

    def dy2_part(c):
        cols = pl.ds(pl.multiple_of(i * 2048 + c * CH, CH), CH)
        return (dacc[:, cols] + drec[:, pl.ds(pl.multiple_of(c * CH, CH), CH)]).astype(BF)

    w2b = w2n[...].astype(BF)

    @pl.loop(0, NCH)
    def _(q):
        c = (q + 2) % NCH
        dh = mm(w2b, dy2_part(c))
        g1[q, 3] = jnp.where(h1t[c].astype(F32) > 0.0, dh, 0.0).astype(BF)
        spread_first(g1, g1_ss, g1_rs, q, q % 2).start()

    @pl.loop(0, NCH)
    def _(c):
        f2[0, 0:128, 0:CP] += mm(h1t[c], dy2_part(c), 1, 1)

    f2[0, 128:136, :] = jnp.broadcast_to(jnp.sum(lossv[...], axis=1, keepdims=True), (8, 128))

    def f2_copy(n):
        rep = (nbx, nby, r)[n]
        core = (i, i, other)[n]
        return remote(f2.at[n], f2r.at[n], f2_ss.at[n], f2_rs.at[n], rep, core)

    f2_copy(0).start()

    @pl.loop(0, NCH + N1)
    def _(t):
        @pl.when(t < NCH)
        def _():
            q = t
            e = q % 2
            spread_first(g1, g1_ss, g1_rs, q, e).wait_recv()
            spread_second(g1, g1_ss, g1_rs, q, e).start()

        for n in range(2):
            @pl.when(t == 3 + 2 * n)
            def _():
                f2_copy(n).wait_recv()
                f2[n + 1] = f2[n] + f2r[n]
                f2_copy(n + 1).start()

        @pl.when(t >= N1)
        def _():
            q = t - N1
            e = q % 2
            slot = q % 4
            spread_second(g1, g1_ss, g1_rs, q, e).wait_recv()

            @pl.when(q >= 4)
            def _():
                rows_copy(0, slot).wait()

            lhs = gathered(g1, q, e)
            eacc[:, half(other)] += mm(lhs, a_s[slot, :, :, half(other)].reshape(4 * CH, 2048))

            @pl.when(q == NCH - 1)
            def _():
                pair_copy(eacc, erec, 1).start()

            eacc[:, half(i)] += mm(lhs, a_s[slot, :, :, half(i)].reshape(4 * CH, 2048))

            @pl.when(q < 4)
            def _():
                rows_copy((q + 6) % NCH, slot).start()

    f2_copy(2).wait_recv()
    pair_copy(eacc, erec, 1).wait_recv()
    dy1 = (eacc[:, half(i)] + erec[...]).astype(BF)
    n_in = dw1_o.shape[0]
    fw[...] = jnp.zeros_like(fw)
    fw[:, 0:n_in] = mm(dy1, x_s[...])
    fw_t = jnp.transpose(fw[...], (1, 0))
    fs[0, 0] = fw_t[0:320]
    fs[0, 1] = fw_t[320:640]

    def pair_half():
        return remote(fs.at[0, other], fr0, fw_ss.at[0], fw_rs.at[0], r, other)

    def quarter(n, h):
        rep = nbx * (1 - (n + h) % 2) + nby * ((n + h) % 2)
        return remote(
            fs.at[1 + n, 0, pl.ds(h * 160, 160)], fr1.at[n, pl.ds(h * 160, 160)],
            fw_ss.at[1 + 2 * n + h], fw_rs.at[1 + 2 * n + h], rep, i,
        )

    def back():
        return remote(fs.at[2, 1], fr2, fw_ss.at[5], fw_rs.at[5], r, other)

    pair_half().start()
    pair_half().wait_recv()
    fs[1, 0] = fs[0, i] + fr0[...]
    for h in range(2):
        quarter(0, h).start()
    for h in range(2):
        quarter(0, h).wait_recv()
        fs[2, 0, h * 160:(h + 1) * 160] = fs[1, 0, h * 160:(h + 1) * 160] + fr1[0, h * 160:(h + 1) * 160]
        quarter(1, h).start()
    for h in range(2):
        quarter(1, h).wait_recv()
    fs[2, 1] = fs[2, 0] + fr1[1]
    back().start()
    f_sum = f2[2] + f2r[2]
    dw2_o[...] = f_sum[0:128, 0:n_class]
    loss_o[...] = f_sum[128:129, 0:1] / count
    back().wait_recv()
    fo[i] = fs[2, 1]
    fo[other] = fr2[...]
    dw1_o[0:320] = fo[0]
    dw1_o[320:n_in] = fo[1, 0:n_in - 320]

    @pl.loop(0, 4)
    def _(b):
        y1_copy(b).wait_send()

    @pl.loop(0, NCH)
    def _(c):
        e = c % 2
        p1_first(c, e).wait_send()
        p1_second(c, e).wait_send()
        y2_copy(c).wait_send()
        z_first(c, e).wait_send()
        z_second(c, e).wait_send()
        spread_first(g2, g2_ss, g2_rs, c, e).wait_send()
        spread_second(g2, g2_ss, g2_rs, c, e).wait_send()
        spread_first(g1, g1_ss, g1_rs, c, e).wait_send()
        spread_second(g1, g1_ss, g1_rs, c, e).wait_send()

    for n in range(3):
        cnt_copy(n).wait_send()
        f2_copy(n).wait_send()
    pair_copy(dacc, drec, 0).wait_send()
    pair_copy(eacc, erec, 1).wait_send()
    pair_half().wait_send()
    for n in range(2):
        for h in range(2):
            quarter(n, h).wait_send()
    back().wait_send()


def solution(mesh):
    def device_step(adj, feat, w1, w2, labels, mask):
        n_in, n_hid = w1.shape
        n_class = w2.shape[1]
        lab = jnp.where(mask > 0, labels, -1).reshape(NCH, CH)
        vmem = pl.BlockSpec(memory_space=pltpu.VMEM)
        hbm = pl.BlockSpec(memory_space=pl.ANY)
        dma = pltpu.SemaphoreType.DMA

        def body(*refs):
            kernel(n_class, *refs)

        loss, dw1, dw2 = pl.pallas_call(
            body,
            out_shape=(
                jax.ShapeDtypeStruct((1, 1), F32),
                jax.ShapeDtypeStruct((n_in, n_hid), F32),
                jax.ShapeDtypeStruct((n_hid, n_class), F32),
            ),
            in_specs=[hbm, hbm, vmem, vmem, vmem],
            out_specs=(vmem, vmem, vmem),
            scratch_shapes=[
                pltpu.VMEM((4, 4, CH, 4096), BF),
                pltpu.VMEM((2048, n_in), BF),
                pltpu.VMEM((128, CP), F32),
                pltpu.VMEM((CP, 128), BF),
                pltpu.VMEM((2, 2048, 128), BF),
                pltpu.VMEM((NCH, 4, CH, 128), F32),
                pltpu.VMEM((NCH, 2, CH, 128), F32),
                pltpu.VMEM((NCH, CH, 128), F32),
                pltpu.VMEM((NCH, 128, CH), BF),
                pltpu.VMEM((NCH, 2, CP, CH), BF),
                pltpu.VMEM((NCH, CP, 4 * CH), F32),
                pltpu.VMEM((NCH, 4, CP, CH), F32),
                pltpu.VMEM((NCH, 2, CP, CH), F32),
                pltpu.VMEM((NCH, CP, CH), F32),
                pltpu.VMEM((NCH, 4, CP, CH), BF),
                pltpu.VMEM((CP, 4096), F32),
                pltpu.VMEM((CP, 2048), F32),
                pltpu.VMEM((NCH, 4, 128, CH), BF),
                pltpu.VMEM((128, 4096), F32),
                pltpu.VMEM((128, 2048), F32),
                pltpu.VMEM((3, 8, 128), F32),
                pltpu.VMEM((3, 8, 128), F32),
                pltpu.VMEM((3, 136, 128), F32),
                pltpu.VMEM((3, 136, 128), F32),
                pltpu.VMEM((128, 640), F32),
                pltpu.VMEM((320, 128), F32),
                pltpu.VMEM((3, 2, 320, 128), F32),
                pltpu.VMEM((2, 320, 128), F32),
                pltpu.VMEM((320, 128), F32),
                pltpu.VMEM((2, 320, 128), F32),
                pltpu.VMEM((1, CH), F32),
                dma((4,)), dma(()),
                dma((4,)), dma((4,)),
                dma((2, NCH)), dma((2, NCH)),
                dma((NCH,)), dma((NCH,)),
                dma((2, NCH)), dma((2, NCH)),
                dma((2, NCH)), dma((2, NCH)),
                dma((2, NCH)), dma((2, NCH)),
                dma((2,)), dma((2,)),
                dma((3,)), dma((3,)),
                dma((3,)), dma((3,)),
                dma((6,)), dma((6,)),
            ],
            compiler_params=pltpu.CompilerParams(
                collective_id=0, has_side_effects=True, vmem_limit_bytes=67043328
            ),
        )(adj, feat, w1, w2, lab)
        return loss.reshape(()), dw1, dw2

    row_spec = P(("rep", "nodes"))
    return jax.shard_map(
        device_step,
        mesh=mesh,
        in_specs=(P(None, "nodes", "rep"), row_spec, P(), P(), row_spec, row_spec),
        out_specs=(P(), P(), P()),
        check_vma=False,
    )
```

```python
import jax
import jax.numpy as jnp
from jax import lax
from jax.experimental import pallas as pl
from jax.experimental.pallas import tpu as pltpu
from jax.sharding import PartitionSpec as P

BF = jnp.bfloat16
F32 = jnp.float32
MESH = pl.DeviceIdType.MESH

CH = 256
NCH = 8
CP = 48
LAGS1 = (2, 4, 5)
LAGS2 = (2, 4, 6, 8)
LAGS3 = (2, 4)
L2, L3, L4 = LAGS1
M1, M2, M3, M4 = LAGS2
N1, N2 = LAGS3


def mm(a, b, ca=1, cb=0):
    return lax.dot_general(a, b, (((ca,), (cb,)), ((), ())), preferred_element_type=F32)


def kernel(
    n_class, adj, feat, w1, w2, lab, msk, loss_o, dw1_o, dw2_o,
    a_s, x_s, w2n, y1, p1, p1r, h1t, y2, zacc, zs, zr, g2, dacc, drec, g1, eacc, erec,
    cnt, cntr, f2, f2r, fr0, fs, fr1, fr2, fo, lossv,
    a_sem, x_sem, y1_ss, y1_rs, p1_ss, p1_rs, y2_ss, y2_rs, z_ss, z_rs, g2_ss, g2_rs, g1_ss, g1_rs,
    d_ss, d_rs, c_ss, c_rs, f2_ss, f2_rs, fw_ss, fw_rs,
):
    r = lax.axis_index("rep")
    i = lax.axis_index("nodes")
    nbx = r + 1 - 2 * (r % 2)
    nby = (r + 2) % 4
    r0, r1 = r % 2, r // 2
    other = 1 - i

    def near(e):
        return nbx * (1 - e) + nby * e

    def far(e):
        return nby * (1 - e) + nbx * e

    def place(a, e):
        d0 = (r0 + a % 2) % 2
        d1 = (r1 + a // 2) % 2
        return 3 * (1 - d0) * (1 - d1) + d0 * (1 - d1) * (1 + e) + (1 - d0) * d1 * (2 - e)

    def remote(src, dst, ss, rs, rep, core):
        return pltpu.make_async_remote_copy(
            src_ref=src, dst_ref=dst, send_sem=ss, recv_sem=rs, device_id=(rep, core), device_id_type=MESH
        )

    def rows_copy(chunk, slot):
        return pltpu.make_async_copy(
            adj.at[:, pl.ds(pl.multiple_of(chunk * CH, CH), CH), :], a_s.at[slot], a_sem.at[slot]
        )

    def cols_start(k, slot):
        @pl.loop(0, NCH)
        def _(g):
            for core in range(2):
                pltpu.make_async_copy(
                    adj.at[:, pl.ds(pl.multiple_of(g * CH, CH), CH), pl.ds(pl.multiple_of(core * 2048 + k * CH, CH), CH)],
                    a_s.at[slot, :, :, pl.ds(pl.multiple_of(g * 2 * CH + core * CH, CH), CH)],
                    a_sem.at[slot],
                ).start()

    x_copy = pltpu.make_async_copy(feat, x_s, x_sem)
    x_copy.start()
    rows_copy(0, 0).start()

    barrier = pltpu.get_barrier_semaphore()
    pl.semaphore_signal(barrier, inc=1, device_id=(nbx, i), device_id_type=MESH)
    pl.semaphore_signal(barrier, inc=1, device_id=(nby, i), device_id_type=MESH)
    pl.semaphore_signal(barrier, inc=1, device_id=(r, other), device_id_type=MESH)

    w2n[...] = jnp.zeros_like(w2n)
    w2n[0:n_class, :] = w2[...]
    w2t = w2n[...].astype(BF)
    total = jnp.sum(jnp.sum(msk[...].astype(F32), axis=0, keepdims=True), axis=1, keepdims=True)
    cnt[0] = jnp.broadcast_to(total, (8, 128))
    w1b = w1[...].astype(BF)
    x_copy.wait()
    for c in range(1, 4):
        rows_copy(c, c).start()

    @pl.loop(0, 4)
    def _(b):
        rows = pl.ds(pl.multiple_of(b * 512, 512), 512)
        y1[i, rows, :] = jnp.transpose(mm(w1b, x_s[:, rows], 0, 0), (1, 0)).astype(BF)

    pl.semaphore_wait(barrier, 3)

    def cnt_copy(n):
        rep = (nbx, nby, r)[n]
        core = (i, i, other)[n]
        return remote(cnt.at[n], cntr.at[n], c_ss.at[n], c_rs.at[n], rep, core)


    def y1_copy(b):
        part = y1.at[i, pl.ds(pl.multiple_of(b * 512, 512), 512), :]
        return remote(part, part, y1_ss.at[b], y1_rs.at[b], r, other)

    def y1_recv(b):
        part = y1.at[other, pl.ds(pl.multiple_of(b * 512, 512), 512), :]
        return remote(part, part, y1_ss.at[b], y1_rs.at[b], r, other)

    @pl.loop(0, 4)
    def _(b):
        y1_copy(b).start()

    cnt_copy(0).start()
    zacc[...] = jnp.zeros_like(zacc)
    dacc[...] = jnp.zeros_like(dacc)
    eacc[...] = jnp.zeros_like(eacc)
    lossv[...] = jnp.zeros_like(lossv)
    f2[0] = jnp.zeros_like(f2[0])
    cnt_copy(0).wait_recv()
    cnt[1] = cnt[0] + cntr[0]
    cnt_copy(1).start()

    @pl.loop(0, 4)
    def _(b):
        y1_recv(b).wait_recv()

    def reduce_copy(buf, rec, ss, rs, n, c, e):
        return remote(buf.at[c, n], rec.at[c, n], ss.at[n, c], rs.at[n, c], far(e) if n == 2 else near(e), i)

    def p1_copy(n, c, e):
        return reduce_copy(p1, p1r, p1_ss, p1_rs, n, c, e)

    def y2_copy(c):
        return remote(y2.at[c, i], y2.at[c, i], y2_ss.at[c], y2_rs.at[c], r, other)

    def y2_recv(c):
        return remote(y2.at[c, other], y2.at[c, other], y2_ss.at[c], y2_rs.at[c], r, other)

    def z_part(lhs, slot, g):
        rhs = a_s[slot, :, :, pl.ds(pl.multiple_of(g * 2 * CH, 2 * CH), 2 * CH)].reshape(4 * CH, 2 * CH)
        return mm(lhs, rhs, 1, 1)

    def pass2_lhs(k):
        return jnp.concatenate([y2[k, 0], y2[k, 1]], axis=1)

    def p1_slot(c):
        return c % 2 + 2 * (1 - c // 4) * ((c // 2) % 2)

    @pl.loop(0, max(NCH - 2 + L4, NCH + L3))
    def _(t):
        @pl.when(t < NCH)
        def _():
            c = t
            e = c % 2
            slot = p1_slot(c)
            rows_copy(c, slot).wait()
            res = mm(a_s[slot].reshape(4 * CH, 4096), y1[...].reshape(4096, 128))
            for a in range(4):
                p1[c, place(a, e)] = res[a * CH:(a + 1) * CH]
            p1_copy(0, c, e).start()
            p1_copy(1, c, e).start()

            @pl.when(jnp.logical_or(c < 2, c == 4))
            def _():
                rows_copy(4 + c - 2 * (c // 4), slot).start()

            @pl.when(c == 5)
            def _():
                rows_copy(7, slot).start()

            @pl.when(jnp.logical_or(c == 2, c == 3))
            def _():
                cols_start(c - 2, slot)

        @pl.when(jnp.logical_and(t >= L2, t < NCH + L2))
        def _():
            c = t - L2
            e = c % 2
            p1_copy(0, c, e).wait_recv()
            p1[c, 2] = p1[c, 2] + p1r[c, 0]
            p1_copy(2, c, e).start()

        @pl.when(jnp.logical_and(t >= L3, t < NCH + L3))
        def _():
            c = t - L3
            e = c % 2
            p1_copy(1, c, e).wait_recv()
            p1_copy(2, c, e).wait_recv()
            h = jnp.maximum(p1[c, 3] + p1r[c, 1] + p1r[c, 2], 0.0)
            ht = jnp.transpose(h, (1, 0)).astype(BF)
            h1t[c] = ht
            y2[c, i] = mm(w2t, ht).astype(BF)
            y2_copy(c).start()

        @pl.when(jnp.logical_and(t >= L4, t < NCH - 2 + L4))
        def _():
            k = t - L4
            slot = 2 + k % 2
            y2_recv(k).wait_recv()
            rows_copy(0, slot).wait()
            lhs = pass2_lhs(k)

            @pl.loop(0, 2)
            def _(gg):
                for g4 in range(4):
                    g = gg * 4 + g4
                    zacc[g] = zacc[g] + z_part(lhs, slot, g)

            cols_start(k + 2, slot)

    def z_copy(n, q, e):
        return reduce_copy(zs, zr, z_ss, z_rs, n, q, e)

    def spread_copy(buf, ss, rs, n, q, e):
        src, dst = ((3, 2), (3, 1), (2, 0))[n]
        return remote(buf.at[q, src], buf.at[q, dst], ss.at[n, q], rs.at[n, q], far(e) if n == 0 else near(e), i)

    def g2_copy(n, q, e):
        return spread_copy(g2, g2_ss, g2_rs, n, q, e)

    def g1_copy(n, q, e):
        return spread_copy(g1, g1_ss, g1_rs, n, q, e)

    cnt_copy(1).wait_recv()
    cnt[2] = cnt[1] + cntr[1]
    cnt_copy(2).start()
    for k in (NCH - 2, NCH - 1):
        y2_recv(k).wait_recv()
        rows_copy(0, 2 + k % 2).wait()
    lhs_6, lhs_7 = pass2_lhs(NCH - 2), pass2_lhs(NCH - 1)
    cnt_copy(2).wait_recv()
    count = (cnt[2] + cntr[2])[0:1, 0:1]
    class_id = lax.broadcasted_iota(jnp.int32, (CP, CH), 0)

    def gathered(buf, q, e):
        return jnp.concatenate([buf[q, place(a, e)] for a in range(4)], axis=1)

    def half(core):
        return pl.ds(pl.multiple_of(core * 2048, 2048), 2048)

    def pair_copy(src, dst, n):
        return remote(src.at[:, half(other)], dst, d_ss.at[n], d_rs.at[n], r, other)

    def p3_slot(q):
        return q % 2 + 2 * (q // 4) * (1 - (q // 2) % 2)

    def p3_chunk(q):
        return (q + 6) % NCH

    def row_of(ref, c):
        return jnp.concatenate([ref[pl.ds(2 * c, 1), :], ref[pl.ds(2 * c + 1, 1), :]], axis=1)

    @pl.loop(0, NCH + M4)
    def _(t):
        @pl.when(t < NCH)
        def _():
            q = t
            e = q % 2
            g = p3_chunk(q)
            z = zacc[g] + z_part(lhs_6, 2, g) + z_part(lhs_7, 3, g)
            for a in range(4):
                zs[q, place(a, e)] = z[:, a * CH:(a + 1) * CH]
            z_copy(0, q, e).start()
            z_copy(1, q, e).start()

            @pl.when(q == NCH - 1)
            def _():
                rows_copy(p3_chunk(4), 2).start()
                rows_copy(p3_chunk(5), 3).start()

        @pl.when(jnp.logical_and(t >= M1, t < NCH + M1))
        def _():
            q = t - M1
            e = q % 2
            z_copy(0, q, e).wait_recv()
            zs[q, 2] = zs[q, 2] + zr[q, 0]
            z_copy(2, q, e).start()

        @pl.when(jnp.logical_and(t >= M2, t < NCH + M2))
        def _():
            q = t - M2
            e = q % 2
            z_copy(1, q, e).wait_recv()
            z_copy(2, q, e).wait_recv()
            z = jnp.where(class_id < n_class, zs[q, 3] + zr[q, 1] + zr[q, 2], -1e30)
            top = jnp.max(z, axis=0, keepdims=True)
            shifted = z - top
            log_p = shifted - jnp.log(jnp.sum(jnp.exp(shifted), axis=0, keepdims=True))
            label = row_of(lab, p3_chunk(q))
            weight = row_of(msk, p3_chunk(q)).astype(F32)
            hit = class_id == label
            lossv[...] = lossv[...] - weight * jnp.sum(jnp.where(hit, log_p, 0.0), axis=0, keepdims=True)
            prob = jnp.exp(log_p)
            g2[q, 3] = ((prob - jnp.where(hit, 1.0, 0.0)) * (weight / count)).astype(BF)
            g2_copy(0, q, e).start()
            g2_copy(1, q, e).start()

        @pl.when(jnp.logical_and(t >= M3, t < NCH + M3))
        def _():
            q = t - M3
            e = q % 2
            g2_copy(0, q, e).wait_recv()
            g2_copy(2, q, e).start()

        @pl.when(t >= M4)
        def _():
            q = t - M4
            e = q % 2
            slot = p3_slot(q)
            g2_copy(1, q, e).wait_recv()
            g2_copy(2, q, e).wait_recv()

            @pl.when(q >= 2)
            def _():
                rows_copy(0, slot).wait()

            lhs = gathered(g2, q, e)
            dacc[:, half(other)] += mm(lhs, a_s[slot, :, :, half(other)].reshape(4 * CH, 2048))

            @pl.when(q == NCH - 1)
            def _():
                pair_copy(dacc, drec, 0).start()

            dacc[:, half(i)] += mm(lhs, a_s[slot, :, :, half(i)].reshape(4 * CH, 2048))

            @pl.when(q < 4)
            def _():
                rows_copy(p3_chunk(q + 2 + 2 * (q // 2)), slot).start()

    pair_copy(dacc, drec, 0).wait_recv()

    def dy2_part(c):
        cols = pl.ds(pl.multiple_of(i * 2048 + c * CH, CH), CH)
        return (dacc[:, cols] + drec[:, pl.ds(pl.multiple_of(c * CH, CH), CH)]).astype(BF)

    def p4_chunk(q):
        return p3_chunk((q + 4) % NCH)

    def f2_copy(n):
        rep = (nbx, nby, r)[n]
        core = (i, i, other)[n]
        return remote(f2.at[n], f2r.at[n], f2_ss.at[n], f2_rs.at[n], rep, core)

    @pl.loop(0, NCH + N2)
    def _(t):
        @pl.when(t < NCH)
        def _():
            q = t
            e = q % 2
            c = p4_chunk(q)
            dy2 = dy2_part(c)
            dh = mm(w2t, dy2, 0, 0)
            g1[q, 3] = jnp.where(h1t[c].astype(F32) > 0.0, dh, 0.0).astype(BF)
            g1_copy(0, q, e).start()
            g1_copy(1, q, e).start()
            f2[0, 0:CP] += mm(dy2, h1t[c], 1, 1)

        @pl.when(jnp.logical_and(t >= N1, t < NCH + N1))
        def _():
            q = t - N1
            e = q % 2
            g1_copy(0, q, e).wait_recv()
            g1_copy(2, q, e).start()

            @pl.when(q == NCH - 1)
            def _():
                f2[0, CP:CP + 8] = jnp.broadcast_to(jnp.sum(lossv[...], axis=1, keepdims=True), (8, 128))
                f2_copy(0).start()

        @pl.when(t >= N2)
        def _():
            q = t - N2
            e = q % 2
            slot = (q + 2) % 4
            g1_copy(1, q, e).wait_recv()
            g1_copy(2, q, e).wait_recv()

            @pl.when(q >= 4)
            def _():
                rows_copy(0, slot).wait()

            lhs = gathered(g1, q, e)
            eacc[:, half(other)] += mm(lhs, a_s[slot, :, :, half(other)].reshape(4 * CH, 2048))

            @pl.when(q == NCH - 1)
            def _():
                pair_copy(eacc, erec, 1).start()

            eacc[:, half(i)] += mm(lhs, a_s[slot, :, :, half(i)].reshape(4 * CH, 2048))

            @pl.when(q < 4)
            def _():
                rows_copy(p4_chunk(q + 4), slot).start()

    f2_copy(0).wait_recv()
    f2[1] = f2[0] + f2r[0]
    f2_copy(1).start()
    pair_copy(eacc, erec, 1).wait_recv()
    dy1 = (eacc[:, half(i)] + erec[...]).astype(BF)
    n_in = dw1_o.shape[0]
    dw = mm(x_s[...], dy1, 1, 1)
    fs[0, 0] = dw[0:320]
    fs[0, 1, n_in - 320 - 2:320] = jnp.zeros((642 - n_in, 128), F32)
    fs[0, 1, 0:n_in - 320] = dw[320:n_in]

    def pair_half():
        return remote(fs.at[0, other], fr0, fw_ss.at[0], fw_rs.at[0], r, other)

    def quarter(n, h):
        rep = nbx * (1 - (n + h) % 2) + nby * ((n + h) % 2)
        return remote(
            fs.at[1 + n, 0, pl.ds(h * 160, 160)], fr1.at[n, pl.ds(h * 160, 160)],
            fw_ss.at[1 + 2 * n + h], fw_rs.at[1 + 2 * n + h], rep, i,
        )

    def back():
        return remote(fs.at[2, 1], fr2, fw_ss.at[5], fw_rs.at[5], r, other)

    pair_half().start()
    pair_half().wait_recv()
    fs[1, 0] = fs[0, i] + fr0[...]
    for h in range(2):
        quarter(0, h).start()
    for h in range(2):
        quarter(0, h).wait_recv()
        fs[2, 0, h * 160:(h + 1) * 160] = fs[1, 0, h * 160:(h + 1) * 160] + fr1[0, h * 160:(h + 1) * 160]
        quarter(1, h).start()
    f2_copy(1).wait_recv()
    f2[2] = f2[1] + f2r[1]
    f2_copy(2).start()
    for h in range(2):
        quarter(1, h).wait_recv()
    fs[2, 1] = fs[2, 0] + fr1[1]
    back().start()
    f2_copy(2).wait_recv()
    f_sum = f2[2] + f2r[2]
    dw2_o[...] = f_sum[0:n_class]
    loss_o[...] = f_sum[CP:CP + 1, 0:1] / count
    back().wait_recv()
    fo[i] = fs[2, 1]
    fo[other] = fr2[...]
    dw1_o[0:320] = fo[0]
    dw1_o[320:n_in] = fo[1, 0:n_in - 320]

    @pl.loop(0, 4)
    def _(b):
        y1_copy(b).wait_send()

    @pl.loop(0, NCH)
    def _(c):
        e = c % 2
        y2_copy(c).wait_send()
        for n in range(3):
            p1_copy(n, c, e).wait_send()
            z_copy(n, c, e).wait_send()
            g2_copy(n, c, e).wait_send()
            g1_copy(n, c, e).wait_send()

    for n in range(3):
        cnt_copy(n).wait_send()
        f2_copy(n).wait_send()
    pair_copy(dacc, drec, 0).wait_send()
    pair_copy(eacc, erec, 1).wait_send()
    pair_half().wait_send()
    for n in range(2):
        for h in range(2):
            quarter(n, h).wait_send()
    back().wait_send()


def emit(*refs):
    for src, dst in zip(refs[:3], refs[3:]):
        dst[...] = src[...]


def solution(mesh):
    def device_step(adj, feat, w1, w2, labels, mask):
        n_in, n_hid = w1.shape
        n_class = w2.shape[1]
        vmem = pl.BlockSpec(memory_space=pltpu.VMEM)
        hbm = pl.BlockSpec(memory_space=pl.ANY)
        dma = pltpu.SemaphoreType.DMA

        def body(*refs):
            kernel(n_class, *refs)

        sums = pl.pallas_call(
            body,
            out_shape=(
                jax.ShapeDtypeStruct((1, 1), F32),
                jax.ShapeDtypeStruct((n_in, n_hid), F32),
                jax.ShapeDtypeStruct((n_class, n_hid), F32),
            ),
            in_specs=[hbm, hbm, vmem, vmem, vmem, vmem],
            out_specs=(vmem, vmem, vmem),
            scratch_shapes=[
                pltpu.VMEM((4, 4, CH, 4096), BF),
                pltpu.VMEM((n_in, 2048), BF),
                pltpu.VMEM((CP, 128), F32),
                pltpu.VMEM((2, 2048, 128), BF),
                pltpu.VMEM((NCH, 4, CH, 128), F32),
                pltpu.VMEM((NCH, 3, CH, 128), F32),
                pltpu.VMEM((NCH, 128, CH), BF),
                pltpu.VMEM((NCH, 2, CP, CH), BF),
                pltpu.VMEM((NCH, CP, 4 * CH), F32),
                pltpu.VMEM((NCH, 4, CP, CH), F32),
                pltpu.VMEM((NCH, 3, CP, CH), F32),
                pltpu.VMEM((NCH, 4, CP, CH), BF),
                pltpu.VMEM((CP, 4096), F32),
                pltpu.VMEM((CP, 2048), F32),
                pltpu.VMEM((NCH, 4, 128, CH), BF),
                pltpu.VMEM((128, 4096), F32),
                pltpu.VMEM((128, 2048), F32),
                pltpu.VMEM((3, 8, 128), F32),
                pltpu.VMEM((3, 8, 128), F32),
                pltpu.VMEM((3, CP + 8, 128), F32),
                pltpu.VMEM((3, CP + 8, 128), F32),
                pltpu.VMEM((320, 128), F32),
                pltpu.VMEM((3, 2, 320, 128), F32),
                pltpu.VMEM((2, 320, 128), F32),
                pltpu.VMEM((320, 128), F32),
                pltpu.VMEM((2, 320, 128), F32),
                pltpu.VMEM((1, CH), F32),
                dma((4,)), dma(()),
                dma((4,)), dma((4,)),
                dma((3, NCH)), dma((3, NCH)),
                dma((NCH,)), dma((NCH,)),
                dma((3, NCH)), dma((3, NCH)),
                dma((3, NCH)), dma((3, NCH)),
                dma((3, NCH)), dma((3, NCH)),
                dma((2,)), dma((2,)),
                dma((3,)), dma((3,)),
                dma((3,)), dma((3,)),
                dma((6,)), dma((6,)),
            ],
            compiler_params=pltpu.CompilerParams(
                collective_id=0, has_side_effects=True, vmem_limit_bytes=67043328
            ),
        )(adj, feat.T, w1, w2.T, labels.reshape(16, 128), mask.reshape(16, 128))
        loss, dw1, dw2 = pl.pallas_call(
            emit,
            out_shape=tuple(jax.ShapeDtypeStruct(x.shape, x.dtype) for x in sums),
            in_specs=[vmem] * 3,
            out_specs=(vmem, vmem, vmem),
        )(*sums)
        return loss.reshape(()), dw1, dw2.T

    row_spec = P(("rep", "nodes"))
    return jax.shard_map(
        device_step,
        mesh=mesh,
        in_specs=(P(None, "nodes", "rep"), row_spec, P(), P(), row_spec, row_spec),
        out_specs=(P(), P(), P()),
        check_vma=False,
    )
```

```python
import jax
import jax.numpy as jnp
from jax import lax
from jax.experimental import pallas as pl
from jax.experimental.pallas import tpu as pltpu
from jax.sharding import PartitionSpec as P

BF = jnp.bfloat16
F32 = jnp.float32
MESH = pl.DeviceIdType.MESH

CH = 256
NCH = 8
CP = 48
HID = 128
ND = 2048
NCOL = 2 * ND
HR = 304
QR = HR // 2
LAGS1 = (2, 4, 5)
LAGS2 = (2, 4, 6, 8)
LAGS3 = (0, 1, 3)
L2, L3, L4 = LAGS1
M1, M2, M3, M4 = LAGS2
N1, N2, N3 = LAGS3
LN = 1
LZ = 1
LG = 1
LB = 1
NROW = 4


def mm(a, b, ca=1, cb=0):
    return lax.dot_general(a, b, (((ca,), (cb,)), ((), ())), preferred_element_type=F32)


def kernel(
    n_class, adj, feat, w1, w2, lab, msk, loss_o, dw1_o, dw2_o,
    a_s, x_s, w2n, y1, p1, p1r, h1t, y2, zacc, zs, zr, g2, dacc, drec, g1, eacc, erec,
    cnt, cntr, f2, f2r, fr0, fs, fr1, lossv,
    a_sem, piece_sem, x_sem, y1_ss, y1_rs, p1_ss, p1_rs, y2_ss, y2_rs, z_ss, z_rs, g2_ss, g2_rs, g1_ss, g1_rs,
    dp_ss, dp_rs, d_ss, d_rs, c_ss, c_rs, f2_ss, f2_rs, fw_ss, fw_rs,
):
    r = lax.axis_index("rep")
    i = lax.axis_index("nodes")
    nbx = r + 1 - 2 * (r % 2)
    nby = (r + 2) % 4
    r0, r1 = r % 2, r // 2
    other = 1 - i

    def near(e):
        return nbx * (1 - e) + nby * e

    def far(e):
        return nby * (1 - e) + nbx * e

    def place(a, e):
        d0 = (r0 + a % 2) % 2
        d1 = (r1 + a // 2) % 2
        return 3 * (1 - d0) * (1 - d1) + d0 * (1 - d1) * (1 + e) + (1 - d0) * d1 * (2 - e)

    def remote(src, dst, ss, rs, rep, core):
        return pltpu.make_async_remote_copy(
            src_ref=src, dst_ref=dst, send_sem=ss, recv_sem=rs, device_id=(rep, core), device_id_type=MESH
        )

    def rows_copy(chunk, slot):
        return pltpu.make_async_copy(
            adj.at[:, pl.ds(pl.multiple_of(chunk * CH, CH), CH), :], a_s.at[slot], a_sem.at[slot]
        )

    def cols_start(k, slot, sem_of):
        @pl.loop(0, NCH)
        def _(n):
            g = (n + 6) % NCH
            for core in range(2):
                pltpu.make_async_copy(
                    adj.at[:, pl.ds(pl.multiple_of(g * CH, CH), CH), pl.ds(pl.multiple_of(core * ND + k * CH, CH), CH)],
                    a_s.at[slot, :, :, pl.ds(pl.multiple_of(g * 2 * CH + core * CH, CH), CH)],
                    sem_of(g),
                ).start()

    def cols_piece_wait(slot, g):
        pltpu.make_async_copy(
            adj.at[:, pl.ds(0, CH), pl.ds(0, 2 * CH)],
            a_s.at[slot, :, :, pl.ds(pl.multiple_of(g * 2 * CH, 2 * CH), 2 * CH)],
            piece_sem.at[slot - 2, g],
        ).wait()

    x_copy = pltpu.make_async_copy(feat, x_s, x_sem)
    x_copy.start()
    rows_copy(0, 0).start()

    barrier = pltpu.get_barrier_semaphore()
    pl.semaphore_signal(barrier, inc=1, device_id=(nbx, i), device_id_type=MESH)
    pl.semaphore_signal(barrier, inc=1, device_id=(nby, i), device_id_type=MESH)
    pl.semaphore_signal(barrier, inc=1, device_id=(r, other), device_id_type=MESH)

    w2n[...] = jnp.zeros_like(w2n)
    w2n[0:n_class, :] = w2[...]
    w2t = w2n[...].astype(BF)
    total = jnp.sum(jnp.sum(msk[...].astype(F32), axis=0, keepdims=True), axis=1, keepdims=True)
    cnt[0] = jnp.broadcast_to(total, (8, HID))
    w1b = w1[...].astype(BF)
    x_copy.wait()
    for c in range(1, 4):
        rows_copy(c, c).start()

    @pl.loop(0, 4)
    def _(b):
        rows = pl.ds(pl.multiple_of(b * 512, 512), 512)
        y1[i, rows, :] = jnp.transpose(mm(w1b, x_s[:, rows], 0, 0), (1, 0)).astype(BF)

    pl.semaphore_wait(barrier, 3)

    def cnt_copy(n):
        rep = (nbx, nby, r)[n]
        core = (i, i, other)[n]
        return remote(cnt.at[n], cntr.at[n], c_ss.at[n], c_rs.at[n], rep, core)


    def y1_copy(b):
        part = y1.at[i, pl.ds(pl.multiple_of(b * 512, 512), 512), :]
        return remote(part, part, y1_ss.at[b], y1_rs.at[b], r, other)

    def y1_recv(b):
        part = y1.at[other, pl.ds(pl.multiple_of(b * 512, 512), 512), :]
        return remote(part, part, y1_ss.at[b], y1_rs.at[b], r, other)

    @pl.loop(0, 4)
    def _(b):
        y1_copy(b).start()

    cnt_copy(0).start()
    zacc[...] = jnp.zeros_like(zacc)
    dacc[...] = jnp.zeros_like(dacc)
    eacc[...] = jnp.zeros_like(eacc)
    lossv[...] = jnp.zeros_like(lossv)
    f2[0] = jnp.zeros_like(f2[0])
    @pl.loop(0, 4)
    def _(b):
        y1_recv(b).wait_recv()

    def reduce_copy(buf, rec, ss, rs, n, c, e):
        return remote(buf.at[c, n], rec.at[c, n], ss.at[n, c], rs.at[n, c], far(e) if n == 2 else near(e), i)

    def p1_copy(n, c, e):
        return reduce_copy(p1, p1r, p1_ss, p1_rs, n, c, e)

    def y2_copy(c):
        return remote(y2.at[c, i], y2.at[c, i], y2_ss.at[c], y2_rs.at[c], r, other)

    def y2_recv(c):
        return remote(y2.at[c, other], y2.at[c, other], y2_ss.at[c], y2_rs.at[c], r, other)

    def z_part(lhs, slot, g):
        rhs = a_s[slot, :, :, pl.ds(pl.multiple_of(g * 2 * CH, 2 * CH), 2 * CH)].reshape(4 * CH, 2 * CH)
        return mm(lhs, rhs, 1, 1)

    def pass2_lhs(k):
        return jnp.concatenate([y2[k, 0], y2[k, 1]], axis=1)

    def p1_slot(c):
        return c % 2 + 2 * (1 - c // 4) * ((c // 2) % 2)

    @pl.loop(0, max(NCH - 2 + L4, NCH + L3))
    def _(t):
        @pl.when(t < NCH)
        def _():
            c = t
            e = c % 2
            slot = p1_slot(c)
            rows_copy(c, slot).wait()
            res = mm(a_s[slot].reshape(4 * CH, NCOL), y1[...].reshape(NCOL, HID))
            for a in range(4):
                p1[c, place(a, e)] = res[a * CH:(a + 1) * CH]
            p1_copy(0, c, e).start()
            if LB == 0:
                p1_copy(1, c, e).start()

            @pl.when(jnp.logical_or(c < 2, c == 4))
            def _():
                rows_copy(4 + c - 2 * (c // 4), slot).start()

            @pl.when(c == 5)
            def _():
                rows_copy(7, slot).start()

            @pl.when(jnp.logical_or(c == 2, c == 3))
            def _():
                cols_start(c - 2, slot, lambda g: a_sem.at[slot])

        @pl.when(jnp.logical_and(t >= L2, t < NCH + L2))
        def _():
            c = t - L2
            e = c % 2
            p1_copy(0, c, e).wait_recv()
            p1[c, 2] = p1[c, 2] + p1r[c, 0]
            p1_copy(2, c, e).start()

        if LB:
            @pl.when(jnp.logical_and(t >= LB, t < NCH + LB))
            def _():
                p1_copy(1, t - LB, (t - LB) % 2).start()

        for n in range(2):
            @pl.when(t == 3 + 6 * n)
            def _():
                cnt_copy(n).wait_recv()
                cnt[n + 1] = cnt[n] + cntr[n]
                cnt_copy(n + 1).start()

        @pl.when(jnp.logical_and(t >= L3, t < NCH + L3))
        def _():
            c = t - L3
            e = c % 2
            p1_copy(1, c, e).wait_recv()
            p1_copy(2, c, e).wait_recv()
            h = jnp.maximum(p1[c, 3] + p1r[c, 1] + p1r[c, 2], 0.0)
            ht = jnp.transpose(h, (1, 0)).astype(BF)
            h1t[c] = ht
            y2[c, i] = mm(w2t, ht).astype(BF)
            y2_copy(c).start()

        @pl.when(jnp.logical_and(t >= L4, t < NCH - 2 + L4))
        def _():
            k = t - L4
            slot = 2 + k % 2
            y2_recv(k).wait_recv()
            rows_copy(0, slot).wait()
            lhs = pass2_lhs(k)

            for g in range(NCH):
                zacc[g] = zacc[g] + z_part(lhs, slot, g)

            @pl.when(k < NCH - 4)
            def _():
                cols_start(k + 2, slot, lambda g: a_sem.at[slot])

            @pl.when(k >= NCH - 4)
            def _():
                cols_start(k + 2, slot, lambda g: piece_sem.at[slot - 2, g])

    def z_copy(n, q, e):
        return reduce_copy(zs, zr, z_ss, z_rs, n, q, e)

    def spread_copy(buf, ss, rs, n, q, e):
        src, dst = ((3, 2), (3, 1), (2, 0))[n]
        return remote(buf.at[q, src], buf.at[q, dst], ss.at[n, q], rs.at[n, q], far(e) if n == 0 else near(e), i)

    def g2_copy(n, q, e):
        return spread_copy(g2, g2_ss, g2_rs, n, q, e)

    def g1_copy(n, q, e):
        return spread_copy(g1, g1_ss, g1_rs, n, q, e)

    for k in (NCH - 2, NCH - 1):
        y2_recv(k).wait_recv()
    lhs_6, lhs_7 = pass2_lhs(NCH - 2), pass2_lhs(NCH - 1)
    cnt_copy(2).wait_recv()
    count = (cnt[2] + cntr[2])[0:1, 0:1]
    class_id = lax.broadcasted_iota(jnp.int32, (CP, CH), 0)

    def gathered(buf, q, e):
        return jnp.concatenate([buf[q, place(a, e)] for a in range(4)], axis=1)

    def half(core):
        return pl.ds(pl.multiple_of(core * ND, ND), ND)

    def pair_copy():
        return remote(eacc.at[:, half(other)], erec, d_ss, d_rs, r, other)

    def p3_slot(q):
        return q % 2 + 2 * (q // 4) * (1 - (q // 2) % 2)

    def p3_chunk(q):
        return (q + 6) % NCH

    def row_of(ref, c):
        return jnp.concatenate([ref[pl.ds(2 * c, 1), :], ref[pl.ds(2 * c + 1, 1), :]], axis=1)

    @pl.loop(0, max(NCH + M3, NROW + M4))
    def _(t):
        @pl.when(t < NCH)
        def _():
            q = t
            e = q % 2
            g = p3_chunk(q)
            cols_piece_wait(2, g)
            cols_piece_wait(3, g)
            z = zacc[g] + z_part(lhs_6, 2, g) + z_part(lhs_7, 3, g)
            for a in range(4):
                zs[q, place(a, e)] = z[:, a * CH:(a + 1) * CH]
            z_copy(0, q, e).start()

            @pl.when(q == NCH - 1)
            def _():
                rows_copy(p3_chunk(4), 2).start()
                rows_copy(p3_chunk(5), 3).start()

        @pl.when(jnp.logical_and(t >= M1, t < NCH + M1))
        def _():
            q = t - M1
            e = q % 2
            z_copy(0, q, e).wait_recv()
            zs[q, 2] = zs[q, 2] + zr[q, 0]
            z_copy(2, q, e).start()

        @pl.when(jnp.logical_and(t >= LZ, t < NCH + LZ))
        def _():
            z_copy(1, t - LZ, (t - LZ) % 2).start()

        @pl.when(jnp.logical_and(t >= M2, t < NCH + M2))
        def _():
            q = t - M2
            e = q % 2
            z_copy(1, q, e).wait_recv()
            z_copy(2, q, e).wait_recv()
            z = jnp.where(class_id < n_class, zs[q, 3] + zr[q, 1] + zr[q, 2], -1e30)
            top = jnp.max(z, axis=0, keepdims=True)
            shifted = z - top
            log_p = shifted - jnp.log(jnp.sum(jnp.exp(shifted), axis=0, keepdims=True))
            label = row_of(lab, p3_chunk(q))
            weight = row_of(msk, p3_chunk(q)).astype(F32)
            hit = class_id == label
            lossv[...] = lossv[...] - weight * jnp.sum(jnp.where(hit, log_p, 0.0), axis=0, keepdims=True)
            prob = jnp.exp(log_p)
            g2[q, 3] = ((prob - jnp.where(hit, 1.0, 0.0)) * (weight / count)).astype(BF)
            g2_copy(0, q, e).start()

        @pl.when(jnp.logical_and(t >= M3, t < NCH + M3))
        def _():
            q = t - M3
            e = q % 2
            g2_copy(0, q, e).wait_recv()
            g2_copy(2, q, e).start()

        @pl.when(jnp.logical_and(t >= M2 + LG, t < NCH + M2 + LG))
        def _():
            g2_copy(1, t - M2 - LG, (t - M2 - LG) % 2).start()

        @pl.when(jnp.logical_and(t >= M4, t < NROW + M4))
        def _():
            q = t - M4
            e = q % 2
            slot = p3_slot(q)
            g2_copy(1, q, e).wait_recv()
            g2_copy(2, q, e).wait_recv()

            @pl.when(q >= 2)
            def _():
                rows_copy(0, slot).wait()

            lhs = gathered(g2, q, e)
            dacc[...] += mm(lhs, a_s[slot].reshape(4 * CH, NCOL))

            @pl.when(q < 4)
            def _():
                rows_copy(p3_chunk(q + 2 + 2 * (q // 2)), slot).start()

    for q in range(NROW, NCH):
        g2_copy(1, q, q % 2).wait_recv()
        g2_copy(2, q, q % 2).wait_recv()
        rows_copy(0, p3_slot(q)).wait()

    PW = 2 * CH

    def cols_of(core, pair):
        return pl.ds(pl.multiple_of(core * ND + pair * PW, PW), PW)

    def dacc_copy(pair):
        return remote(dacc.at[:, cols_of(other, pair)], drec.at[pair], dp_ss.at[pair], dp_rs.at[pair], r, other)

    def finish_pass3(core, pair):
        cols = cols_of(core, pair)
        acc = dacc[:, cols]
        for q in range(NROW, NCH):
            acc = acc + mm(gathered(g2, q, q % 2), a_s[p3_slot(q), :, :, cols].reshape(4 * CH, PW))
        dacc[:, cols] = acc

    def p4_chunk(q):
        return p3_chunk((q + 4) % NCH)

    def f2_copy(n):
        rep = (nbx, nby, r)[n]
        core = (i, i, other)[n]
        return remote(f2.at[n], f2r.at[n], f2_ss.at[n], f2_rs.at[n], rep, core)

    NP = NCH // 2

    @pl.loop(0, NP + N3)
    def _(t):
        @pl.when(t < NP)
        def _():
            pair = (t + 1) % NP
            finish_pass3(other, pair)
            dacc_copy(pair).start()
            finish_pass3(i, pair)

        @pl.when(jnp.logical_and(t >= N1, t < NP + N1))
        def _():
            pair = (t - N1 + 1) % NP
            dacc_copy(pair).wait_recv()
            dy2 = (dacc[:, cols_of(i, pair)] + drec[pair]).astype(BF)
            dh = mm(w2t, dy2, 0, 0)
            for e in range(2):
                q = 2 * (t - N1) + e
                part = dh[:, e * CH:(e + 1) * CH]
                g1[q, 3] = jnp.where(h1t[2 * pair + e].astype(F32) > 0.0, part, 0.0).astype(BF)
                g1_copy(0, q, e).start()
            for e in range(2):
                f2[0, 0:CP] += mm(dy2[:, e * CH:(e + 1) * CH], h1t[2 * pair + e], 1, 1)

            @pl.when(t == NP - 1 + N1)
            def _():
                f2[0, CP:CP + 8] = jnp.broadcast_to(jnp.sum(lossv[...], axis=1, keepdims=True), (8, HID))
                f2_copy(0).start()

        @pl.when(jnp.logical_and(t >= LN, t < NP + LN))
        def _():
            for e in range(2):
                g1_copy(1, 2 * (t - LN) + e, e).start()

        @pl.when(jnp.logical_and(t >= N2, t < NP + N2))
        def _():
            for e in range(2):
                q = 2 * (t - N2) + e
                g1_copy(0, q, e).wait_recv()
                g1_copy(2, q, e).start()

        @pl.when(t >= N3)
        def _():
            for e in range(2):
                q = 2 * (t - N3) + e
                slot = (q + 2) % 4
                g1_copy(1, q, e).wait_recv()
                g1_copy(2, q, e).wait_recv()

                @pl.when(q >= 4)
                def _():
                    rows_copy(0, slot).wait()

                lhs = gathered(g1, q, e)

                @pl.when(q < NCH - 1)
                def _():
                    eacc[...] += mm(lhs, a_s[slot].reshape(4 * CH, NCOL))

                if e == 1:

                    @pl.when(q == NCH - 1)
                    def _():
                        for core in (other, i):
                            cols = half(core)
                            eacc[:, cols] += mm(lhs, a_s[slot, :, :, cols].reshape(4 * CH, ND))
                            if core is other:
                                pair_copy().start()

                @pl.when(q < 4)
                def _():
                    rows_copy(p4_chunk(q + 4), slot).start()

    f2_copy(0).wait_recv()
    f2[1] = f2[0] + f2r[0]
    f2_copy(1).start()
    pair_copy().wait_recv()
    dy1 = (eacc[:, half(i)] + erec[...]).astype(BF)
    n_in = w1.shape[0]
    dw = mm(x_s[...], dy1, 1, 1)
    fs[0, 0] = dw[:HR]
    fs[0, 1, HR - 8:] = jnp.zeros((8, HID), F32)
    fs[0, 1, :n_in - HR] = dw[HR:]

    def pair_half():
        return remote(fs.at[0, other], fr0, fw_ss.at[0], fw_rs.at[0], r, other)

    def quarter(n, h):
        rep = nbx * (1 - (n + h) % 2) + nby * ((n + h) % 2)
        return remote(
            fs.at[1 + n, 0, pl.ds(h * QR, QR)], fr1.at[n, pl.ds(h * QR, QR)],
            fw_ss.at[1 + 2 * n + h], fw_rs.at[1 + 2 * n + h], rep, i,
        )

    def back():
        return remote(fs.at[2, 1], dw1_o.at[i], fw_ss.at[5], fw_rs.at[5], r, other)

    def back_recv():
        return remote(fs.at[2, 1], dw1_o.at[other], fw_ss.at[5], fw_rs.at[5], r, other)

    pair_half().start()
    pair_half().wait_recv()
    fs[1, 0] = fs[0, i] + fr0[...]
    for h in range(2):
        quarter(0, h).start()
    for h in range(2):
        quarter(0, h).wait_recv()
        rows = pl.ds(h * QR, QR)
        fs[2, 0, rows] = fs[1, 0, rows] + fr1[0, rows]
        quarter(1, h).start()
    f2_copy(1).wait_recv()
    f2[2] = f2[1] + f2r[1]
    f2_copy(2).start()
    for h in range(2):
        quarter(1, h).wait_recv()
    fs[2, 1] = fs[2, 0] + fr1[1]
    back().start()
    keep = pltpu.make_async_copy(fs.at[2, 1], dw1_o.at[i], x_sem)
    keep.start()
    f2_copy(2).wait_recv()
    f_sum = f2[2] + f2r[2]
    dw2_o[...] = f_sum[0:n_class]
    loss_o[...] = f_sum[CP:CP + 1, 0:1] / count
    keep.wait()
    back_recv().wait_recv()

    @pl.loop(0, 4)
    def _(b):
        y1_copy(b).wait_send()

    @pl.loop(0, NCH)
    def _(c):
        e = c % 2
        y2_copy(c).wait_send()
        for n in range(3):
            p1_copy(n, c, e).wait_send()
            z_copy(n, c, e).wait_send()
            g2_copy(n, c, e).wait_send()
            g1_copy(n, c, e).wait_send()

    for pair in range(NCH // 2):
        dacc_copy(pair).wait_send()
    for n in range(3):
        cnt_copy(n).wait_send()
        f2_copy(n).wait_send()
    pair_copy().wait_send()
    pair_half().wait_send()
    for n in range(2):
        for h in range(2):
            quarter(n, h).wait_send()
    back().wait_send()


def emit(loss, dw1, dw2, loss_o, dw1_o, dw2_o):
    loss_o[...] = loss[...]
    dw2_o[...] = dw2[...]
    dw1_o[:HR] = dw1[0]
    dw1_o[HR:] = dw1[1, :dw1_o.shape[0] - HR]


def solution(mesh):
    def device_step(adj, feat, w1, w2, labels, mask):
        n_in, n_hid = w1.shape
        n_class = w2.shape[1]
        vmem = pl.BlockSpec(memory_space=pltpu.VMEM)
        hbm = pl.BlockSpec(memory_space=pl.ANY)
        dma = pltpu.SemaphoreType.DMA
        per = (3, NCH)

        def body(*refs):
            kernel(n_class, *refs)

        sums = pl.pallas_call(
            body,
            out_shape=(
                jax.ShapeDtypeStruct((1, 1), F32),
                jax.ShapeDtypeStruct((2, HR, n_hid), F32),
                jax.ShapeDtypeStruct((n_class, n_hid), F32),
            ),
            in_specs=[hbm, hbm, vmem, vmem, vmem, vmem],
            out_specs=(vmem, hbm, vmem),
            scratch_shapes=[
                pltpu.VMEM((4, 4, CH, NCOL), BF),
                pltpu.VMEM((n_in, ND), BF),
                pltpu.VMEM((CP, HID), F32),
                pltpu.VMEM((2, ND, HID), BF),
                pltpu.VMEM((NCH, 4, CH, HID), F32),
                pltpu.VMEM((NCH, 3, CH, HID), F32),
                pltpu.VMEM((NCH, HID, CH), BF),
                pltpu.VMEM((NCH, 2, CP, CH), BF),
                pltpu.VMEM((NCH, CP, 4 * CH), F32),
                pltpu.VMEM((NCH, 4, CP, CH), F32),
                pltpu.VMEM((NCH, 3, CP, CH), F32),
                pltpu.VMEM((NCH, 4, CP, CH), BF),
                pltpu.VMEM((CP, NCOL), F32),
                pltpu.VMEM((NCH // 2, CP, 2 * CH), F32),
                pltpu.VMEM((NCH, 4, HID, CH), BF),
                pltpu.VMEM((HID, NCOL), F32),
                pltpu.VMEM((HID, ND), F32),
                pltpu.VMEM((3, 8, HID), F32),
                pltpu.VMEM((3, 8, HID), F32),
                pltpu.VMEM((3, CP + 8, HID), F32),
                pltpu.VMEM((3, CP + 8, HID), F32),
                pltpu.VMEM((HR, HID), F32),
                pltpu.VMEM((3, 2, HR, HID), F32),
                pltpu.VMEM((2, HR, HID), F32),
                pltpu.VMEM((1, CH), F32),
                dma((4,)), dma((2, NCH)), dma(()),
                *[
                    dma(n) for n in ((4,), per, (NCH,), per, per, per, (NCH // 2,), (), (3,), (3,), (6,))
                    for _ in ("send", "receive")
                ],
            ],
            compiler_params=pltpu.CompilerParams(
                collective_id=0, has_side_effects=True, vmem_limit_bytes=67043328
            ),
        )(adj, feat.T, w1, w2.T, labels.reshape(-1, HID), mask.reshape(-1, HID))
        loss, dw1, dw2 = pl.pallas_call(
            emit,
            out_shape=(
                jax.ShapeDtypeStruct((1, 1), F32),
                jax.ShapeDtypeStruct((n_in, n_hid), F32),
                jax.ShapeDtypeStruct((n_class, n_hid), F32),
            ),
            in_specs=[vmem] * 3,
            out_specs=(vmem, vmem, vmem),
        )(*sums)
        return loss.reshape(()), dw1, dw2.T

    row_spec = P(("rep", "nodes"))
    return jax.shard_map(
        device_step,
        mesh=mesh,
        in_specs=(P(None, "nodes", "rep"), row_spec, P(), P(), row_spec, row_spec),
        out_specs=(P(), P(), P()),
        check_vma=False,
    )
```

```python
import jax
import jax.numpy as jnp
from jax import lax
from jax.experimental import pallas as pl
from jax.experimental.pallas import tpu as pltpu
from jax.sharding import PartitionSpec as P

BF = jnp.bfloat16
F32 = jnp.float32
MESH = pl.DeviceIdType.MESH

CH = 256
NCH = 8
CP = 48
HID = 128
ND = 2048
NCOL = 2 * ND
HR = 304
QR = HR // 2
LAGS1 = (2, 4, 5)
LAGS2 = (2, 4, 6, 8)
LAGS3 = (0, 1, 3)
L2, L3, L4 = LAGS1
M1, M2, M3, M4 = LAGS2
N1, N2, N3 = LAGS3
LN = 1
LZ = 1
LG = 1
LB = 1
NROW = 4


def mm(a, b, ca=1, cb=0):
    return lax.dot_general(a, b, (((ca,), (cb,)), ((), ())), preferred_element_type=F32)


def kernel(
    n_class, adj, feat, w1_h, w2_h, lab_h, msk_h, dw1_o, rest_o, w1, w2, lab, msk, rest,
    a_s, x_s, w2n, y1, p1, p1r, h1t, y2, zacc, zs, zr, g2, dacc, drec, g1, eacc, erec,
    cnt, cntr, f2, f2r, fr0, fs, fr1, lossv,
    a_sem, piece_sem, x_sem, in_sem, y1_ss, y1_rs, p1_ss, p1_rs, y2_ss, y2_rs, z_ss, z_rs, g2_ss, g2_rs, g1_ss, g1_rs,
    dp_ss, dp_rs, d_ss, d_rs, c_ss, c_rs, f2_ss, f2_rs, fw_ss, fw_rs,
):
    r = lax.axis_index("rep")
    i = lax.axis_index("nodes")
    nbx = r + 1 - 2 * (r % 2)
    nby = (r + 2) % 4
    r0, r1 = r % 2, r // 2
    other = 1 - i

    def near(e):
        return nbx * (1 - e) + nby * e

    def far(e):
        return nby * (1 - e) + nbx * e

    def place(a, e):
        d0 = (r0 + a % 2) % 2
        d1 = (r1 + a // 2) % 2
        return 3 * (1 - d0) * (1 - d1) + d0 * (1 - d1) * (1 + e) + (1 - d0) * d1 * (2 - e)

    def remote(src, dst, ss, rs, rep, core):
        return pltpu.make_async_remote_copy(
            src_ref=src, dst_ref=dst, send_sem=ss, recv_sem=rs, device_id=(rep, core), device_id_type=MESH
        )

    def rows_copy(chunk, slot):
        return pltpu.make_async_copy(
            adj.at[:, pl.ds(pl.multiple_of(chunk * CH, CH), CH), :], a_s.at[slot], a_sem.at[slot]
        )

    def cols_start(k, slot, sem_of):
        @pl.loop(0, NCH)
        def _(n):
            g = (n + 6) % NCH
            for core in range(2):
                pltpu.make_async_copy(
                    adj.at[:, pl.ds(pl.multiple_of(g * CH, CH), CH), pl.ds(pl.multiple_of(core * ND + k * CH, CH), CH)],
                    a_s.at[slot, :, :, pl.ds(pl.multiple_of(g * 2 * CH + core * CH, CH), CH)],
                    sem_of(g),
                ).start()

    def cols_piece_wait(slot, g):
        pltpu.make_async_copy(
            adj.at[:, pl.ds(0, CH), pl.ds(0, 2 * CH)],
            a_s.at[slot, :, :, pl.ds(pl.multiple_of(g * 2 * CH, 2 * CH), 2 * CH)],
            piece_sem.at[slot - 2, g],
        ).wait()

    x_copy = pltpu.make_async_copy(feat, x_s, x_sem)
    x_copy.start()
    small = [
        pltpu.make_async_copy(src, dst, in_sem.at[n])
        for n, (src, dst) in enumerate(((w1_h, w1), (w2_h, w2), (lab_h, lab), (msk_h, msk)))
    ]
    for copy in small:
        copy.start()
    rows_copy(0, 0).start()

    barrier = pltpu.get_barrier_semaphore()
    pl.semaphore_signal(barrier, inc=1, device_id=(nbx, i), device_id_type=MESH)
    pl.semaphore_signal(barrier, inc=1, device_id=(nby, i), device_id_type=MESH)
    pl.semaphore_signal(barrier, inc=1, device_id=(r, other), device_id_type=MESH)

    for copy in small:
        copy.wait()
    w2n[...] = jnp.zeros_like(w2n)
    w2n[0:n_class, :] = w2[...]
    w2t = w2n[...].astype(BF)
    total = jnp.sum(jnp.sum(msk[...].astype(F32), axis=0, keepdims=True), axis=1, keepdims=True)
    cnt[0] = jnp.broadcast_to(total, (8, HID))
    w1b = w1[...].astype(BF)
    x_copy.wait()
    for c in range(1, 4):
        rows_copy(c, c).start()

    @pl.loop(0, 4)
    def _(b):
        rows = pl.ds(pl.multiple_of(b * 512, 512), 512)
        y1[i, rows, :] = jnp.transpose(mm(w1b, x_s[:, rows], 0, 0), (1, 0)).astype(BF)

    pl.semaphore_wait(barrier, 3)

    def cnt_copy(n):
        rep = (nbx, nby, r)[n]
        core = (i, i, other)[n]
        return remote(cnt.at[n], cntr.at[n], c_ss.at[n], c_rs.at[n], rep, core)


    def y1_copy(b):
        part = y1.at[i, pl.ds(pl.multiple_of(b * 512, 512), 512), :]
        return remote(part, part, y1_ss.at[b], y1_rs.at[b], r, other)

    def y1_recv(b):
        part = y1.at[other, pl.ds(pl.multiple_of(b * 512, 512), 512), :]
        return remote(part, part, y1_ss.at[b], y1_rs.at[b], r, other)

    @pl.loop(0, 4)
    def _(b):
        y1_copy(b).start()

    cnt_copy(0).start()
    zacc[...] = jnp.zeros_like(zacc)
    dacc[...] = jnp.zeros_like(dacc)
    eacc[...] = jnp.zeros_like(eacc)
    lossv[...] = jnp.zeros_like(lossv)
    f2[0] = jnp.zeros_like(f2[0])
    @pl.loop(0, 4)
    def _(b):
        y1_recv(b).wait_recv()

    def reduce_copy(buf, rec, ss, rs, n, c, e):
        return remote(buf.at[c, n], rec.at[c, n], ss.at[n, c], rs.at[n, c], far(e) if n == 2 else near(e), i)

    def p1_copy(n, c, e):
        return reduce_copy(p1, p1r, p1_ss, p1_rs, n, c, e)

    def y2_copy(c):
        return remote(y2.at[c, i], y2.at[c, i], y2_ss.at[c], y2_rs.at[c], r, other)

    def y2_recv(c):
        return remote(y2.at[c, other], y2.at[c, other], y2_ss.at[c], y2_rs.at[c], r, other)

    def z_part(lhs, slot, g):
        rhs = a_s[slot, :, :, pl.ds(pl.multiple_of(g * 2 * CH, 2 * CH), 2 * CH)].reshape(4 * CH, 2 * CH)
        return mm(lhs, rhs, 1, 1)

    def pass2_lhs(k):
        return jnp.concatenate([y2[k, 0], y2[k, 1]], axis=1)

    def p1_slot(c):
        return c % 2 + 2 * (1 - c // 4) * ((c // 2) % 2)

    @pl.loop(0, max(NCH - 2 + L4, NCH + L3))
    def _(t):
        @pl.when(t < NCH)
        def _():
            c = t
            e = c % 2
            slot = p1_slot(c)
            rows_copy(c, slot).wait()
            res = mm(a_s[slot].reshape(4 * CH, NCOL), y1[...].reshape(NCOL, HID))
            for a in range(4):
                p1[c, place(a, e)] = res[a * CH:(a + 1) * CH]
            p1_copy(0, c, e).start()
            if LB == 0:
                p1_copy(1, c, e).start()

            @pl.when(jnp.logical_or(c < 2, c == 4))
            def _():
                rows_copy(4 + c - 2 * (c // 4), slot).start()

            @pl.when(c == 5)
            def _():
                rows_copy(7, slot).start()

            @pl.when(jnp.logical_or(c == 2, c == 3))
            def _():
                cols_start(c - 2, slot, lambda g: a_sem.at[slot])

        @pl.when(jnp.logical_and(t >= L2, t < NCH + L2))
        def _():
            c = t - L2
            e = c % 2
            p1_copy(0, c, e).wait_recv()
            p1[c, 2] = p1[c, 2] + p1r[c, 0]
            p1_copy(2, c, e).start()

        if LB:
            @pl.when(jnp.logical_and(t >= LB, t < NCH + LB))
            def _():
                p1_copy(1, t - LB, (t - LB) % 2).start()

        for n in range(2):
            @pl.when(t == 3 + 6 * n)
            def _():
                cnt_copy(n).wait_recv()
                cnt[n + 1] = cnt[n] + cntr[n]
                cnt_copy(n + 1).start()

        @pl.when(jnp.logical_and(t >= L3, t < NCH + L3))
        def _():
            c = t - L3
            e = c % 2
            p1_copy(1, c, e).wait_recv()
            p1_copy(2, c, e).wait_recv()
            h = jnp.maximum(p1[c, 3] + p1r[c, 1] + p1r[c, 2], 0.0)
            ht = jnp.transpose(h, (1, 0)).astype(BF)
            h1t[c] = ht
            y2[c, i] = mm(w2t, ht).astype(BF)
            y2_copy(c).start()

        @pl.when(jnp.logical_and(t >= L4, t < NCH - 2 + L4))
        def _():
            k = t - L4
            slot = 2 + k % 2
            y2_recv(k).wait_recv()
            rows_copy(0, slot).wait()
            lhs = pass2_lhs(k)

            for g in range(NCH):
                zacc[g] = zacc[g] + z_part(lhs, slot, g)

            @pl.when(k < NCH - 4)
            def _():
                cols_start(k + 2, slot, lambda g: a_sem.at[slot])

            @pl.when(k >= NCH - 4)
            def _():
                cols_start(k + 2, slot, lambda g: piece_sem.at[slot - 2, g])

    def z_copy(n, q, e):
        return reduce_copy(zs, zr, z_ss, z_rs, n, q, e)

    def spread_copy(buf, ss, rs, n, q, e):
        src, dst = ((3, 2), (3, 1), (2, 0))[n]
        return remote(buf.at[q, src], buf.at[q, dst], ss.at[n, q], rs.at[n, q], far(e) if n == 0 else near(e), i)

    def g2_copy(n, q, e):
        return spread_copy(g2, g2_ss, g2_rs, n, q, e)

    def g1_copy(n, q, e):
        return spread_copy(g1, g1_ss, g1_rs, n, q, e)

    for k in (NCH - 2, NCH - 1):
        y2_recv(k).wait_recv()
    lhs_6, lhs_7 = pass2_lhs(NCH - 2), pass2_lhs(NCH - 1)
    cnt_copy(2).wait_recv()
    count = (cnt[2] + cntr[2])[0:1, 0:1]
    class_id = lax.broadcasted_iota(jnp.int32, (CP, CH), 0)

    def gathered(buf, q, e):
        return jnp.concatenate([buf[q, place(a, e)] for a in range(4)], axis=1)

    def half(core):
        return pl.ds(pl.multiple_of(core * ND, ND), ND)

    def pair_copy():
        return remote(eacc.at[:, half(other)], erec, d_ss, d_rs, r, other)

    def p3_slot(q):
        return q % 2 + 2 * (q // 4) * (1 - (q // 2) % 2)

    def p3_chunk(q):
        return (q + 6) % NCH

    def row_of(ref, c):
        return jnp.concatenate([ref[pl.ds(2 * c, 1), :], ref[pl.ds(2 * c + 1, 1), :]], axis=1)

    @pl.loop(0, max(NCH + M3, NROW + M4))
    def _(t):
        @pl.when(t < NCH)
        def _():
            q = t
            e = q % 2
            g = p3_chunk(q)
            cols_piece_wait(2, g)
            cols_piece_wait(3, g)
            z = zacc[g] + z_part(lhs_6, 2, g) + z_part(lhs_7, 3, g)
            for a in range(4):
                zs[q, place(a, e)] = z[:, a * CH:(a + 1) * CH]
            z_copy(0, q, e).start()

            @pl.when(q == NCH - 1)
            def _():
                rows_copy(p3_chunk(4), 2).start()
                rows_copy(p3_chunk(5), 3).start()

        @pl.when(jnp.logical_and(t >= M1, t < NCH + M1))
        def _():
            q = t - M1
            e = q % 2
            z_copy(0, q, e).wait_recv()
            zs[q, 2] = zs[q, 2] + zr[q, 0]
            z_copy(2, q, e).start()

        @pl.when(jnp.logical_and(t >= LZ, t < NCH + LZ))
        def _():
            z_copy(1, t - LZ, (t - LZ) % 2).start()

        @pl.when(jnp.logical_and(t >= M2, t < NCH + M2))
        def _():
            q = t - M2
            e = q % 2
            z_copy(1, q, e).wait_recv()
            z_copy(2, q, e).wait_recv()
            z = jnp.where(class_id < n_class, zs[q, 3] + zr[q, 1] + zr[q, 2], -1e30)
            top = jnp.max(z, axis=0, keepdims=True)
            shifted = z - top
            log_p = shifted - jnp.log(jnp.sum(jnp.exp(shifted), axis=0, keepdims=True))
            label = row_of(lab, p3_chunk(q))
            weight = row_of(msk, p3_chunk(q)).astype(F32)
            hit = class_id == label
            lossv[...] = lossv[...] - weight * jnp.sum(jnp.where(hit, log_p, 0.0), axis=0, keepdims=True)
            prob = jnp.exp(log_p)
            g2[q, 3] = ((prob - jnp.where(hit, 1.0, 0.0)) * (weight / count)).astype(BF)
            g2_copy(0, q, e).start()

        @pl.when(jnp.logical_and(t >= M3, t < NCH + M3))
        def _():
            q = t - M3
            e = q % 2
            g2_copy(0, q, e).wait_recv()
            g2_copy(2, q, e).start()

        @pl.when(jnp.logical_and(t >= M2 + LG, t < NCH + M2 + LG))
        def _():
            g2_copy(1, t - M2 - LG, (t - M2 - LG) % 2).start()

        @pl.when(jnp.logical_and(t >= M4, t < NROW + M4))
        def _():
            q = t - M4
            e = q % 2
            slot = p3_slot(q)
            g2_copy(1, q, e).wait_recv()
            g2_copy(2, q, e).wait_recv()

            @pl.when(q >= 2)
            def _():
                rows_copy(0, slot).wait()

            lhs = gathered(g2, q, e)
            dacc[...] += mm(lhs, a_s[slot].reshape(4 * CH, NCOL))

            @pl.when(q < 4)
            def _():
                rows_copy(p3_chunk(q + 2 + 2 * (q // 2)), slot).start()

    for q in range(NROW, NCH):
        g2_copy(1, q, q % 2).wait_recv()
        g2_copy(2, q, q % 2).wait_recv()
        rows_copy(0, p3_slot(q)).wait()

    PW = 2 * CH

    def cols_of(core, pair):
        return pl.ds(pl.multiple_of(core * ND + pair * PW, PW), PW)

    def dacc_copy(pair):
        return remote(dacc.at[:, cols_of(other, pair)], drec.at[pair], dp_ss.at[pair], dp_rs.at[pair], r, other)

    def finish_pass3(core, pair):
        cols = cols_of(core, pair)
        acc = dacc[:, cols]
        for q in range(NROW, NCH):
            acc = acc + mm(gathered(g2, q, q % 2), a_s[p3_slot(q), :, :, cols].reshape(4 * CH, PW))
        dacc[:, cols] = acc

    def p4_chunk(q):
        return p3_chunk((q + 4) % NCH)

    def f2_copy(n):
        rep = (nbx, nby, r)[n]
        core = (i, i, other)[n]
        return remote(f2.at[n], f2r.at[n], f2_ss.at[n], f2_rs.at[n], rep, core)

    NP = NCH // 2

    @pl.loop(0, NP + N3)
    def _(t):
        @pl.when(t < NP)
        def _():
            pair = (t + 1) % NP
            finish_pass3(other, pair)
            dacc_copy(pair).start()
            finish_pass3(i, pair)

        @pl.when(jnp.logical_and(t >= N1, t < NP + N1))
        def _():
            pair = (t - N1 + 1) % NP
            dacc_copy(pair).wait_recv()
            dy2 = (dacc[:, cols_of(i, pair)] + drec[pair]).astype(BF)
            dh = mm(w2t, dy2, 0, 0)
            for e in range(2):
                q = 2 * (t - N1) + e
                part = dh[:, e * CH:(e + 1) * CH]
                g1[q, 3] = jnp.where(h1t[2 * pair + e].astype(F32) > 0.0, part, 0.0).astype(BF)
                g1_copy(0, q, e).start()
            for e in range(2):
                f2[0, 0:CP] += mm(dy2[:, e * CH:(e + 1) * CH], h1t[2 * pair + e], 1, 1)

            @pl.when(t == NP - 1 + N1)
            def _():
                f2[0, CP:CP + 8] = jnp.broadcast_to(jnp.sum(lossv[...], axis=1, keepdims=True), (8, HID))
                f2_copy(0).start()

        @pl.when(jnp.logical_and(t >= LN, t < NP + LN))
        def _():
            for e in range(2):
                g1_copy(1, 2 * (t - LN) + e, e).start()

        @pl.when(jnp.logical_and(t >= N2, t < NP + N2))
        def _():
            for e in range(2):
                q = 2 * (t - N2) + e
                g1_copy(0, q, e).wait_recv()
                g1_copy(2, q, e).start()

        @pl.when(t >= N3)
        def _():
            for e in range(2):
                q = 2 * (t - N3) + e
                slot = (q + 2) % 4
                g1_copy(1, q, e).wait_recv()
                g1_copy(2, q, e).wait_recv()

                @pl.when(q >= 4)
                def _():
                    rows_copy(0, slot).wait()

                lhs = gathered(g1, q, e)

                @pl.when(q < NCH - 1)
                def _():
                    eacc[...] += mm(lhs, a_s[slot].reshape(4 * CH, NCOL))

                if e == 1:

                    @pl.when(q == NCH - 1)
                    def _():
                        for core in (other, i):
                            cols = half(core)
                            eacc[:, cols] += mm(lhs, a_s[slot, :, :, cols].reshape(4 * CH, ND))
                            if core is other:
                                pair_copy().start()

                @pl.when(q < 4)
                def _():
                    rows_copy(p4_chunk(q + 4), slot).start()

    f2_copy(0).wait_recv()
    f2[1] = f2[0] + f2r[0]
    f2_copy(1).start()
    pair_copy().wait_recv()
    dy1 = (eacc[:, half(i)] + erec[...]).astype(BF)
    n_in = w1.shape[0]
    dw = mm(x_s[...], dy1, 1, 1)
    fs[0, 0] = dw[:HR]
    fs[0, 1, HR - 8:] = jnp.zeros((8, HID), F32)
    fs[0, 1, :n_in - HR] = dw[HR:]

    def pair_half():
        return remote(fs.at[0, other], fr0, fw_ss.at[0], fw_rs.at[0], r, other)

    def quarter(n, h):
        rep = nbx * (1 - (n + h) % 2) + nby * ((n + h) % 2)
        return remote(
            fs.at[1 + n, 0, pl.ds(h * QR, QR)], fr1.at[n, pl.ds(h * QR, QR)],
            fw_ss.at[1 + 2 * n + h], fw_rs.at[1 + 2 * n + h], rep, i,
        )

    def back():
        return remote(fs.at[2, 1], dw1_o.at[i], fw_ss.at[5], fw_rs.at[5], r, other)

    def back_recv():
        return remote(fs.at[2, 1], dw1_o.at[other], fw_ss.at[5], fw_rs.at[5], r, other)

    pair_half().start()
    pair_half().wait_recv()
    fs[1, 0] = fs[0, i] + fr0[...]
    for h in range(2):
        quarter(0, h).start()
    for h in range(2):
        quarter(0, h).wait_recv()
        rows = pl.ds(h * QR, QR)
        fs[2, 0, rows] = fs[1, 0, rows] + fr1[0, rows]
        quarter(1, h).start()
    f2_copy(1).wait_recv()
    f2[2] = f2[1] + f2r[1]
    f2_copy(2).start()
    for h in range(2):
        quarter(1, h).wait_recv()
    fs[2, 1] = fs[2, 0] + fr1[1]
    back().start()
    keep = pltpu.make_async_copy(fs.at[2, 1], dw1_o.at[i], x_sem)
    keep.start()
    f2_copy(2).wait_recv()
    rest[0:CP] = f2[2, 0:CP] + f2r[2, 0:CP]
    rest[CP:CP + 8] = (f2[2, CP:CP + 8] + f2r[2, CP:CP + 8]) / count
    rest_copy = pltpu.make_async_copy(rest, rest_o, in_sem.at[0])
    rest_copy.start()
    keep.wait()
    rest_copy.wait()
    back_recv().wait_recv()

    @pl.loop(0, 4)
    def _(b):
        y1_copy(b).wait_send()

    @pl.loop(0, NCH)
    def _(c):
        e = c % 2
        y2_copy(c).wait_send()
        for n in range(3):
            p1_copy(n, c, e).wait_send()
            z_copy(n, c, e).wait_send()
            g2_copy(n, c, e).wait_send()
            g1_copy(n, c, e).wait_send()

    for pair in range(NCH // 2):
        dacc_copy(pair).wait_send()
    for n in range(3):
        cnt_copy(n).wait_send()
        f2_copy(n).wait_send()
    pair_copy().wait_send()
    pair_half().wait_send()
    for n in range(2):
        for h in range(2):
            quarter(n, h).wait_send()
    back().wait_send()


def emit(dw1, rest, loss_o, dw1_o, dw2_o):
    loss_o[...] = rest[CP:CP + 1, 0:1]
    dw2_o[...] = rest[:dw2_o.shape[0]]
    dw1_o[:HR] = dw1[0]
    dw1_o[HR:] = dw1[1, :dw1_o.shape[0] - HR]


def solution(mesh):
    def device_step(adj, feat, w1, w2, labels, mask):
        n_in, n_hid = w1.shape
        n_class = w2.shape[1]
        vmem = pl.BlockSpec(memory_space=pltpu.VMEM)
        hbm = pl.BlockSpec(memory_space=pl.ANY)
        dma = pltpu.SemaphoreType.DMA
        per = (3, NCH)

        def body(*refs):
            kernel(n_class, *refs)

        sums = pl.pallas_call(
            body,
            out_shape=(
                jax.ShapeDtypeStruct((2, HR, n_hid), F32),
                jax.ShapeDtypeStruct((CP + 8, n_hid), F32),
            ),
            in_specs=[hbm] * 6,
            out_specs=(hbm, hbm),
            scratch_shapes=[
                pltpu.VMEM((n_in, HID), F32),
                pltpu.VMEM((n_class, HID), F32),
                pltpu.VMEM((ND // HID, HID), jnp.int32),
                pltpu.VMEM((ND // HID, HID), jnp.int32),
                pltpu.VMEM((CP + 8, HID), F32),
                pltpu.VMEM((4, 4, CH, NCOL), BF),
                pltpu.VMEM((n_in, ND), BF),
                pltpu.VMEM((CP, HID), F32),
                pltpu.VMEM((2, ND, HID), BF),
                pltpu.VMEM((NCH, 4, CH, HID), F32),
                pltpu.VMEM((NCH, 3, CH, HID), F32),
                pltpu.VMEM((NCH, HID, CH), BF),
                pltpu.VMEM((NCH, 2, CP, CH), BF),
                pltpu.VMEM((NCH, CP, 4 * CH), F32),
                pltpu.VMEM((NCH, 4, CP, CH), F32),
                pltpu.VMEM((NCH, 3, CP, CH), F32),
                pltpu.VMEM((NCH, 4, CP, CH), BF),
                pltpu.VMEM((CP, NCOL), F32),
                pltpu.VMEM((NCH // 2, CP, 2 * CH), F32),
                pltpu.VMEM((NCH, 4, HID, CH), BF),
                pltpu.VMEM((HID, NCOL), F32),
                pltpu.VMEM((HID, ND), F32),
                pltpu.VMEM((3, 8, HID), F32),
                pltpu.VMEM((3, 8, HID), F32),
                pltpu.VMEM((3, CP + 8, HID), F32),
                pltpu.VMEM((3, CP + 8, HID), F32),
                pltpu.VMEM((HR, HID), F32),
                pltpu.VMEM((3, 2, HR, HID), F32),
                pltpu.VMEM((2, HR, HID), F32),
                pltpu.VMEM((1, CH), F32),
                dma((4,)), dma((2, NCH)), dma(()), dma((4,)),
                *[
                    dma(n) for n in ((4,), per, (NCH,), per, per, per, (NCH // 2,), (), (3,), (3,), (6,))
                    for _ in ("send", "receive")
                ],
            ],
            compiler_params=pltpu.CompilerParams(
                collective_id=0, has_side_effects=True, vmem_limit_bytes=67043328
            ),
        )(adj, feat.T, w1, w2.T, labels.reshape(-1, HID), mask.reshape(-1, HID))
        loss, dw1, dw2 = pl.pallas_call(
            emit,
            out_shape=(
                jax.ShapeDtypeStruct((1, 1), F32),
                jax.ShapeDtypeStruct((n_in, n_hid), F32),
                jax.ShapeDtypeStruct((n_class, n_hid), F32),
            ),
            in_specs=[vmem] * 2,
            out_specs=(vmem, vmem, vmem),
        )(*sums)
        return loss.reshape(()), dw1, dw2.T

    row_spec = P(("rep", "nodes"))
    return jax.shard_map(
        device_step,
        mesh=mesh,
        in_specs=(P(None, "nodes", "rep"), row_spec, P(), P(), row_spec, row_spec),
        out_specs=(P(), P(), P()),
        check_vma=False,
    )
```

```python
import jax
import jax.numpy as jnp
from jax import lax
from jax.experimental import pallas as pl
from jax.experimental.pallas import tpu as pltpu
from jax.sharding import PartitionSpec as P

BF = jnp.bfloat16
F32 = jnp.float32
MESH = pl.DeviceIdType.MESH

CH = 256
NCH = 8
CP = 48
HID = 128
ND = 2048
NCOL = 2 * ND
HR = 304
QR = HR // 2
LAGS1 = (2, 4, 5)
LAGS2 = (2, 4, 6, 8)
LAGS3 = (0, 1, 3)
L2, L3, L4 = LAGS1
M1, M2, M3, M4 = LAGS2
N1, N2, N3 = LAGS3
LN = 1
LZ = 0
LG = 1
LB = 1
NROW = 4


def mm(a, b, ca=1, cb=0):
    return lax.dot_general(a, b, (((ca,), (cb,)), ((), ())), preferred_element_type=F32)


def kernel(
    n_class, adj, feat, w1_h, w2_h, lab_h, msk_h, dw1_o, rest_o, w1, w2, lab, msk, rest,
    a_s, x_s, w2n, y1, p1, p1r, h1t, y2, zacc, zs, zr, g2, dacc, drec, g1, eacc, erec,
    cnt, cntr, f2, f2r, fr0, fs, fr1, lossv,
    a_sem, piece_sem, x_sem, in_sem, y1_ss, y1_rs, p1_ss, p1_rs, y2_ss, y2_rs, z_ss, z_rs, g2_ss, g2_rs, g1_ss, g1_rs,
    dp_ss, dp_rs, d_ss, d_rs, c_ss, c_rs, f2_ss, f2_rs, fw_ss, fw_rs,
):
    r = lax.axis_index("rep")
    i = lax.axis_index("nodes")
    nbx = r + 1 - 2 * (r % 2)
    nby = (r + 2) % 4
    r0, r1 = r % 2, r // 2
    other = 1 - i

    def near(e):
        return nbx * (1 - e) + nby * e

    def far(e):
        return nby * (1 - e) + nbx * e

    def place(a, e):
        d0 = (r0 + a % 2) % 2
        d1 = (r1 + a // 2) % 2
        return 3 * (1 - d0) * (1 - d1) + d0 * (1 - d1) * (1 + e) + (1 - d0) * d1 * (2 - e)

    def remote(src, dst, ss, rs, rep, core):
        return pltpu.make_async_remote_copy(
            src_ref=src, dst_ref=dst, send_sem=ss, recv_sem=rs, device_id=(rep, core), device_id_type=MESH
        )

    def rows_copy(chunk, slot):
        return pltpu.make_async_copy(
            adj.at[:, pl.ds(pl.multiple_of(chunk * CH, CH), CH), :], a_s.at[slot], a_sem.at[slot]
        )

    def cols_start(k, slot, sem_of):
        @pl.loop(0, NCH)
        def _(n):
            g = (n + 6) % NCH
            for core in range(2):
                pltpu.make_async_copy(
                    adj.at[:, pl.ds(pl.multiple_of(g * CH, CH), CH), pl.ds(pl.multiple_of(core * ND + k * CH, CH), CH)],
                    a_s.at[slot, :, :, pl.ds(pl.multiple_of(g * 2 * CH + core * CH, CH), CH)],
                    sem_of(g),
                ).start()

    def cols_piece_wait(slot, g):
        pltpu.make_async_copy(
            adj.at[:, pl.ds(0, CH), pl.ds(0, 2 * CH)],
            a_s.at[slot, :, :, pl.ds(pl.multiple_of(g * 2 * CH, 2 * CH), 2 * CH)],
            piece_sem.at[slot - 2, g],
        ).wait()

    x_copy = pltpu.make_async_copy(feat, x_s, x_sem)
    x_copy.start()
    small = [
        pltpu.make_async_copy(src, dst, in_sem.at[n])
        for n, (src, dst) in enumerate(((w1_h, w1), (w2_h, w2), (lab_h, lab), (msk_h, msk)))
    ]
    for copy in small:
        copy.start()
    rows_copy(0, 0).start()

    barrier = pltpu.get_barrier_semaphore()
    pl.semaphore_signal(barrier, inc=1, device_id=(nbx, i), device_id_type=MESH)
    pl.semaphore_signal(barrier, inc=1, device_id=(nby, i), device_id_type=MESH)
    pl.semaphore_signal(barrier, inc=1, device_id=(r, other), device_id_type=MESH)

    for copy in small:
        copy.wait()
    w2n[...] = jnp.zeros_like(w2n)
    w2n[0:n_class, :] = w2[...]
    w2t = w2n[...].astype(BF)
    total = jnp.sum(jnp.sum(msk[...].astype(F32), axis=0, keepdims=True), axis=1, keepdims=True)
    cnt[0] = jnp.broadcast_to(total, (8, HID))
    w1b = w1[...].astype(BF)
    x_copy.wait()
    for c in range(1, 4):
        rows_copy(c, c).start()

    @pl.loop(0, 4)
    def _(b):
        rows = pl.ds(pl.multiple_of(b * 512, 512), 512)
        y1[i, rows, :] = jnp.transpose(mm(w1b, x_s[:, rows], 0, 0), (1, 0)).astype(BF)

    pl.semaphore_wait(barrier, 3)

    def cnt_copy(n):
        rep = (nbx, nby, r)[n]
        core = (i, i, other)[n]
        return remote(cnt.at[n], cntr.at[n], c_ss.at[n], c_rs.at[n], rep, core)


    def y1_copy(b):
        part = y1.at[i, pl.ds(pl.multiple_of(b * 512, 512), 512), :]
        return remote(part, part, y1_ss.at[b], y1_rs.at[b], r, other)

    def y1_recv(b):
        part = y1.at[other, pl.ds(pl.multiple_of(b * 512, 512), 512), :]
        return remote(part, part, y1_ss.at[b], y1_rs.at[b], r, other)

    @pl.loop(0, 4)
    def _(b):
        y1_copy(b).start()

    cnt_copy(0).start()
    zacc[...] = jnp.zeros_like(zacc)
    dacc[...] = jnp.zeros_like(dacc)
    eacc[...] = jnp.zeros_like(eacc)
    lossv[...] = jnp.zeros_like(lossv)
    f2[0] = jnp.zeros_like(f2[0])
    @pl.loop(0, 4)
    def _(b):
        y1_recv(b).wait_recv()

    def reduce_copy(buf, rec, ss, rs, n, c, e):
        return remote(buf.at[c, n], rec.at[c, n], ss.at[n, c], rs.at[n, c], far(e) if n == 2 else near(e), i)

    def p1_copy(n, c, e):
        return reduce_copy(p1, p1r, p1_ss, p1_rs, n, c, e)

    def y2_copy(c):
        return remote(y2.at[c, i], y2.at[c, i], y2_ss.at[c], y2_rs.at[c], r, other)

    def y2_recv(c):
        return remote(y2.at[c, other], y2.at[c, other], y2_ss.at[c], y2_rs.at[c], r, other)

    def z_part(lhs, slot, g):
        rhs = a_s[slot, :, :, pl.ds(pl.multiple_of(g * 2 * CH, 2 * CH), 2 * CH)].reshape(4 * CH, 2 * CH)
        return mm(lhs, rhs, 1, 1)

    def pass2_lhs(k):
        return jnp.concatenate([y2[k, 0], y2[k, 1]], axis=1)

    def p1_slot(c):
        return c % 2 + 2 * (1 - c // 4) * ((c // 2) % 2)

    @pl.loop(0, max(NCH - 2 + L4, NCH + L3))
    def _(t):
        @pl.when(t < NCH)
        def _():
            c = t
            e = c % 2
            slot = p1_slot(c)
            rows_copy(c, slot).wait()
            res = mm(a_s[slot].reshape(4 * CH, NCOL), y1[...].reshape(NCOL, HID))
            for a in range(4):
                p1[c, place(a, e)] = res[a * CH:(a + 1) * CH]
            p1_copy(0, c, e).start()
            if LB == 0:
                p1_copy(1, c, e).start()

            @pl.when(jnp.logical_or(c < 2, c == 4))
            def _():
                rows_copy(4 + c - 2 * (c // 4), slot).start()

            @pl.when(c == 5)
            def _():
                rows_copy(7, slot).start()

            @pl.when(jnp.logical_or(c == 2, c == 3))
            def _():
                cols_start(c - 2, slot, lambda g: a_sem.at[slot])

        @pl.when(jnp.logical_and(t >= L2, t < NCH + L2))
        def _():
            c = t - L2
            e = c % 2
            p1_copy(0, c, e).wait_recv()
            p1[c, 2] = p1[c, 2] + p1r[c, 0]
            p1_copy(2, c, e).start()

        if LB:
            @pl.when(jnp.logical_and(t >= LB, t < NCH + LB))
            def _():
                p1_copy(1, t - LB, (t - LB) % 2).start()

        for n in range(2):
            @pl.when(t == 3 + 6 * n)
            def _():
                cnt_copy(n).wait_recv()
                cnt[n + 1] = cnt[n] + cntr[n]
                cnt_copy(n + 1).start()

        @pl.when(jnp.logical_and(t >= L3, t < NCH + L3))
        def _():
            c = t - L3
            e = c % 2
            p1_copy(1, c, e).wait_recv()
            p1_copy(2, c, e).wait_recv()
            h = jnp.maximum(p1[c, 3] + p1r[c, 1] + p1r[c, 2], 0.0)
            ht = jnp.transpose(h, (1, 0)).astype(BF)
            h1t[c] = ht
            y2[c, i] = mm(w2t, ht).astype(BF)
            y2_copy(c).start()

        @pl.when(jnp.logical_and(t >= L4, t < NCH - 2 + L4))
        def _():
            k = t - L4
            slot = 2 + k % 2
            y2_recv(k).wait_recv()
            rows_copy(0, slot).wait()
            lhs = pass2_lhs(k)

            for g in range(NCH):
                zacc[g] = zacc[g] + z_part(lhs, slot, g)

            @pl.when(k < NCH - 4)
            def _():
                cols_start(k + 2, slot, lambda g: a_sem.at[slot])

            @pl.when(k >= NCH - 4)
            def _():
                cols_start(k + 2, slot, lambda g: piece_sem.at[slot - 2, g])

    def z_copy(n, q, e):
        return reduce_copy(zs, zr, z_ss, z_rs, n, q, e)

    def spread_copy(buf, ss, rs, n, q, e):
        src, dst = ((3, 2), (3, 1), (2, 0))[n]
        return remote(buf.at[q, src], buf.at[q, dst], ss.at[n, q], rs.at[n, q], far(e) if n == 0 else near(e), i)

    def g2_copy(n, q, e):
        return spread_copy(g2, g2_ss, g2_rs, n, q, e)

    def g1_copy(n, q, e):
        return spread_copy(g1, g1_ss, g1_rs, n, q, e)

    for k in (NCH - 2, NCH - 1):
        y2_recv(k).wait_recv()
    lhs_6, lhs_7 = pass2_lhs(NCH - 2), pass2_lhs(NCH - 1)
    cnt_copy(2).wait_recv()
    count = (cnt[2] + cntr[2])[0:1, 0:1]
    class_id = lax.broadcasted_iota(jnp.int32, (CP, CH), 0)

    def gathered(buf, q, e):
        return jnp.concatenate([buf[q, place(a, e)] for a in range(4)], axis=1)

    def half(core):
        return pl.ds(pl.multiple_of(core * ND, ND), ND)

    def pair_copy():
        return remote(eacc.at[:, half(other)], erec, d_ss, d_rs, r, other)

    def p3_slot(q):
        return q % 2 + 2 * (q // 4) * (1 - (q // 2) % 2)

    def p3_chunk(q):
        return (q + 6) % NCH

    def row_of(ref, c):
        return jnp.concatenate([ref[pl.ds(2 * c, 1), :], ref[pl.ds(2 * c + 1, 1), :]], axis=1)

    @pl.loop(0, max(NCH + M3, NROW + M4))
    def _(t):
        @pl.when(t < NCH)
        def _():
            q = t
            e = q % 2
            g = p3_chunk(q)
            cols_piece_wait(2, g)
            cols_piece_wait(3, g)
            z = zacc[g] + z_part(lhs_6, 2, g) + z_part(lhs_7, 3, g)
            for a in range(4):
                zs[q, place(a, e)] = z[:, a * CH:(a + 1) * CH]
            z_copy(0, q, e).start()

            @pl.when(q == NCH - 1)
            def _():
                rows_copy(p3_chunk(4), 2).start()
                rows_copy(p3_chunk(5), 3).start()

        @pl.when(jnp.logical_and(t >= M1, t < NCH + M1))
        def _():
            q = t - M1
            e = q % 2
            z_copy(0, q, e).wait_recv()
            zs[q, 2] = zs[q, 2] + zr[q, 0]
            z_copy(2, q, e).start()

        @pl.when(jnp.logical_and(t >= LZ, t < NCH + LZ))
        def _():
            z_copy(1, t - LZ, (t - LZ) % 2).start()

        @pl.when(jnp.logical_and(t >= M2, t < NCH + M2))
        def _():
            q = t - M2
            e = q % 2
            z_copy(1, q, e).wait_recv()
            z_copy(2, q, e).wait_recv()
            z = jnp.where(class_id < n_class, zs[q, 3] + zr[q, 1] + zr[q, 2], -1e30)
            top = jnp.max(z, axis=0, keepdims=True)
            shifted = z - top
            log_p = shifted - jnp.log(jnp.sum(jnp.exp(shifted), axis=0, keepdims=True))
            label = row_of(lab, p3_chunk(q))
            weight = row_of(msk, p3_chunk(q)).astype(F32)
            hit = class_id == label
            lossv[...] = lossv[...] - weight * jnp.sum(jnp.where(hit, log_p, 0.0), axis=0, keepdims=True)
            prob = jnp.exp(log_p)
            g2[q, 3] = ((prob - jnp.where(hit, 1.0, 0.0)) * (weight / count)).astype(BF)
            g2_copy(0, q, e).start()

        @pl.when(jnp.logical_and(t >= M3, t < NCH + M3))
        def _():
            q = t - M3
            e = q % 2
            g2_copy(0, q, e).wait_recv()
            g2_copy(2, q, e).start()

        @pl.when(jnp.logical_and(t >= M2 + LG, t < NCH + M2 + LG))
        def _():
            g2_copy(1, t - M2 - LG, (t - M2 - LG) % 2).start()

        @pl.when(jnp.logical_and(t >= M4, t < NROW + M4))
        def _():
            q = t - M4
            e = q % 2
            slot = p3_slot(q)
            g2_copy(1, q, e).wait_recv()
            g2_copy(2, q, e).wait_recv()

            @pl.when(q >= 2)
            def _():
                rows_copy(0, slot).wait()

            lhs = gathered(g2, q, e)
            dacc[...] += mm(lhs, a_s[slot].reshape(4 * CH, NCOL))

            @pl.when(q < 4)
            def _():
                rows_copy(p3_chunk(q + 2 + 2 * (q // 2)), slot).start()

    for q in range(NROW, NCH):
        g2_copy(1, q, q % 2).wait_recv()
        g2_copy(2, q, q % 2).wait_recv()
        rows_copy(0, p3_slot(q)).wait()

    PW = 2 * CH

    def cols_of(core, pair):
        return pl.ds(pl.multiple_of(core * ND + pair * PW, PW), PW)

    def dacc_copy(pair):
        return remote(dacc.at[:, cols_of(other, pair)], drec.at[pair], dp_ss.at[pair], dp_rs.at[pair], r, other)

    def finish_pass3(core, pair):
        cols = cols_of(core, pair)
        acc = dacc[:, cols]
        for q in range(NROW, NCH):
            acc = acc + mm(gathered(g2, q, q % 2), a_s[p3_slot(q), :, :, cols].reshape(4 * CH, PW))
        dacc[:, cols] = acc

    def p4_chunk(q):
        return p3_chunk((q + 4) % NCH)

    def f2_copy(n):
        rep = (nbx, nby, r)[n]
        core = (i, i, other)[n]
        return remote(f2.at[n], f2r.at[n], f2_ss.at[n], f2_rs.at[n], rep, core)

    NP = NCH // 2

    @pl.loop(0, NP + N3)
    def _(t):
        @pl.when(t < NP)
        def _():
            pair = (t + 1) % NP
            finish_pass3(other, pair)
            dacc_copy(pair).start()
            finish_pass3(i, pair)

        @pl.when(jnp.logical_and(t >= N1, t < NP + N1))
        def _():
            pair = (t - N1 + 1) % NP
            dacc_copy(pair).wait_recv()
            dy2 = (dacc[:, cols_of(i, pair)] + drec[pair]).astype(BF)
            dh = mm(w2t, dy2, 0, 0)
            for e in range(2):
                q = 2 * (t - N1) + e
                part = dh[:, e * CH:(e + 1) * CH]
                g1[q, 3] = jnp.where(h1t[2 * pair + e].astype(F32) > 0.0, part, 0.0).astype(BF)
                g1_copy(0, q, e).start()
            for e in range(2):
                f2[0, 0:CP] += mm(dy2[:, e * CH:(e + 1) * CH], h1t[2 * pair + e], 1, 1)

            @pl.when(t == NP - 1 + N1)
            def _():
                f2[0, CP:CP + 8] = jnp.broadcast_to(jnp.sum(lossv[...], axis=1, keepdims=True), (8, HID))
                f2_copy(0).start()

        @pl.when(jnp.logical_and(t >= LN, t < NP + LN))
        def _():
            for e in range(2):
                g1_copy(1, 2 * (t - LN) + e, e).start()

        @pl.when(jnp.logical_and(t >= N2, t < NP + N2))
        def _():
            for e in range(2):
                q = 2 * (t - N2) + e
                g1_copy(0, q, e).wait_recv()
                g1_copy(2, q, e).start()

        @pl.when(t >= N3)
        def _():
            for e in range(2):
                q = 2 * (t - N3) + e
                slot = (q + 2) % 4
                g1_copy(1, q, e).wait_recv()
                g1_copy(2, q, e).wait_recv()

                @pl.when(q >= 4)
                def _():
                    rows_copy(0, slot).wait()

                lhs = gathered(g1, q, e)

                @pl.when(q < NCH - 1)
                def _():
                    eacc[...] += mm(lhs, a_s[slot].reshape(4 * CH, NCOL))

                if e == 1:

                    @pl.when(q == NCH - 1)
                    def _():
                        for core in (other, i):
                            cols = half(core)
                            eacc[:, cols] += mm(lhs, a_s[slot, :, :, cols].reshape(4 * CH, ND))
                            if core is other:
                                pair_copy().start()

                @pl.when(q < 4)
                def _():
                    rows_copy(p4_chunk(q + 4), slot).start()

    f2_copy(0).wait_recv()
    f2[1] = f2[0] + f2r[0]
    f2_copy(1).start()
    pair_copy().wait_recv()
    dy1 = (eacc[:, half(i)] + erec[...]).astype(BF)
    n_in = w1.shape[0]
    dw = mm(x_s[...], dy1, 1, 1)
    fs[0, 0] = dw[:HR]
    fs[0, 1, HR - 8:] = jnp.zeros((8, HID), F32)
    fs[0, 1, :n_in - HR] = dw[HR:]

    def pair_half():
        return remote(fs.at[0, other], fr0, fw_ss.at[0], fw_rs.at[0], r, other)

    def quarter(n, h):
        rep = nbx * (1 - (n + h) % 2) + nby * ((n + h) % 2)
        return remote(
            fs.at[1 + n, 0, pl.ds(h * QR, QR)], fr1.at[n, pl.ds(h * QR, QR)],
            fw_ss.at[1 + 2 * n + h], fw_rs.at[1 + 2 * n + h], rep, i,
        )

    def back():
        return remote(fs.at[2, 1], dw1_o.at[i], fw_ss.at[5], fw_rs.at[5], r, other)

    def back_recv():
        return remote(fs.at[2, 1], dw1_o.at[other], fw_ss.at[5], fw_rs.at[5], r, other)

    pair_half().start()
    pair_half().wait_recv()
    fs[1, 0] = fs[0, i] + fr0[...]
    for h in range(2):
        quarter(0, h).start()
    for h in range(2):
        quarter(0, h).wait_recv()
        rows = pl.ds(h * QR, QR)
        fs[2, 0, rows] = fs[1, 0, rows] + fr1[0, rows]
        quarter(1, h).start()
    f2_copy(1).wait_recv()
    f2[2] = f2[1] + f2r[1]
    f2_copy(2).start()
    for h in range(2):
        quarter(1, h).wait_recv()
    fs[2, 1] = fs[2, 0] + fr1[1]
    back().start()
    keep = pltpu.make_async_copy(fs.at[2, 1], dw1_o.at[i], x_sem)
    keep.start()
    f2_copy(2).wait_recv()
    rest[0:CP] = f2[2, 0:CP] + f2r[2, 0:CP]
    rest[CP:CP + 8] = (f2[2, CP:CP + 8] + f2r[2, CP:CP + 8]) / count
    rest_copy = pltpu.make_async_copy(rest, rest_o, in_sem.at[0])
    rest_copy.start()
    keep.wait()
    rest_copy.wait()
    back_recv().wait_recv()

    @pl.loop(0, 4)
    def _(b):
        y1_copy(b).wait_send()

    @pl.loop(0, NCH)
    def _(c):
        e = c % 2
        y2_copy(c).wait_send()
        for n in range(3):
            p1_copy(n, c, e).wait_send()
            z_copy(n, c, e).wait_send()
            g2_copy(n, c, e).wait_send()
            g1_copy(n, c, e).wait_send()

    for pair in range(NCH // 2):
        dacc_copy(pair).wait_send()
    for n in range(3):
        cnt_copy(n).wait_send()
        f2_copy(n).wait_send()
    pair_copy().wait_send()
    pair_half().wait_send()
    for n in range(2):
        for h in range(2):
            quarter(n, h).wait_send()
    back().wait_send()


def emit(dw1, rest, loss_o, dw1_o, dw2_o):
    loss_o[...] = rest[CP:CP + 1, 0:1]
    dw2_o[...] = rest[:dw2_o.shape[0]]
    dw1_o[:HR] = dw1[0]
    dw1_o[HR:] = dw1[1, :dw1_o.shape[0] - HR]


def solution(mesh):
    def device_step(adj, feat, w1, w2, labels, mask):
        n_in, n_hid = w1.shape
        n_class = w2.shape[1]
        vmem = pl.BlockSpec(memory_space=pltpu.VMEM)
        hbm = pl.BlockSpec(memory_space=pl.ANY)
        dma = pltpu.SemaphoreType.DMA
        per = (3, NCH)

        def body(*refs):
            kernel(n_class, *refs)

        sums = pl.pallas_call(
            body,
            out_shape=(
                jax.ShapeDtypeStruct((2, HR, n_hid), F32),
                jax.ShapeDtypeStruct((CP + 8, n_hid), F32),
            ),
            in_specs=[hbm] * 6,
            out_specs=(hbm, hbm),
            scratch_shapes=[
                pltpu.VMEM((n_in, HID), F32),
                pltpu.VMEM((n_class, HID), F32),
                pltpu.VMEM((ND // HID, HID), jnp.int32),
                pltpu.VMEM((ND // HID, HID), jnp.int32),
                pltpu.VMEM((CP + 8, HID), F32),
                pltpu.VMEM((4, 4, CH, NCOL), BF),
                pltpu.VMEM((n_in, ND), BF),
                pltpu.VMEM((CP, HID), F32),
                pltpu.VMEM((2, ND, HID), BF),
                pltpu.VMEM((NCH, 4, CH, HID), F32),
                pltpu.VMEM((NCH, 3, CH, HID), F32),
                pltpu.VMEM((NCH, HID, CH), BF),
                pltpu.VMEM((NCH, 2, CP, CH), BF),
                pltpu.VMEM((NCH, CP, 4 * CH), F32),
                pltpu.VMEM((NCH, 4, CP, CH), F32),
                pltpu.VMEM((NCH, 3, CP, CH), F32),
                pltpu.VMEM((NCH, 4, CP, CH), BF),
                pltpu.VMEM((CP, NCOL), F32),
                pltpu.VMEM((NCH // 2, CP, 2 * CH), F32),
                pltpu.VMEM((NCH, 4, HID, CH), BF),
                pltpu.VMEM((HID, NCOL), F32),
                pltpu.VMEM((HID, ND), F32),
                pltpu.VMEM((3, 8, HID), F32),
                pltpu.VMEM((3, 8, HID), F32),
                pltpu.VMEM((3, CP + 8, HID), F32),
                pltpu.VMEM((3, CP + 8, HID), F32),
                pltpu.VMEM((HR, HID), F32),
                pltpu.VMEM((3, 2, HR, HID), F32),
                pltpu.VMEM((2, HR, HID), F32),
                pltpu.VMEM((1, CH), F32),
                dma((4,)), dma((2, NCH)), dma(()), dma((4,)),
                *[
                    dma(n) for n in ((4,), per, (NCH,), per, per, per, (NCH // 2,), (), (3,), (3,), (6,))
                    for _ in ("send", "receive")
                ],
            ],
            compiler_params=pltpu.CompilerParams(
                collective_id=0, has_side_effects=True, vmem_limit_bytes=67043328
            ),
        )(adj, feat.T, w1, w2.T, labels.reshape(-1, HID), mask.reshape(-1, HID))
        loss, dw1, dw2 = pl.pallas_call(
            emit,
            out_shape=(
                jax.ShapeDtypeStruct((1, 1), F32),
                jax.ShapeDtypeStruct((n_in, n_hid), F32),
                jax.ShapeDtypeStruct((n_class, n_hid), F32),
            ),
            in_specs=[vmem] * 2,
            out_specs=(vmem, vmem, vmem),
        )(*sums)
        return loss.reshape(()), dw1, dw2.T

    row_spec = P(("rep", "nodes"))
    return jax.shard_map(
        device_step,
        mesh=mesh,
        in_specs=(P(None, "nodes", "rep"), row_spec, P(), P(), row_spec, row_spec),
        out_specs=(P(), P(), P()),
        check_vma=False,
    )
```
